256 devices in a mesh: gx: 8 (over y, x_hi), gy: 32 (over z, x_lo, core).
Axes of the slice: x: 4 (x_hi: 2, x_lo: 2; x = x_hi * 2 + x_lo), y: 4, z: 8, core: 2. Of those that a mesh axis runs over, the one named last changes fastest.
Arguments:
- species_means: bfloat16 [8, 64, 120, 1024], P(None, 'gy', None, 'gx'), may hold values from 0.19921875 to 5
- zonal_edge_velocity: float32 [64, 120, 1024], P('gy', None, 'gx'), may hold values from -6 to 6
- meridional_edge_velocity: float32 [64, 120, 1024], P('gy', None, 'gx'), may hold values from -6 to 6
- scaled_warmth: float32 [64, 120, 1024], P('gy', None, 'gx'), may hold values from 0.5 to 2
- donor_depths: float32 [64, 120, 1024], P('gy', None, 'gx'), may hold values from 0.5 to 2
- leading_donor_level: int32 [64, 120, 1024], P('gy', None, 'gx'), may hold values from 0 to 118, as said below
- opening_share: bfloat16 [64, 120, 1024], P('gy', None, 'gx'), may hold values from 0 to 0.44921875
- closing_share: bfloat16 [64, 120, 1024], P('gy', None, 'gx'), may hold values from 0.546875 to 1
Outputs:
- tracers_out: float32 [8, 64, 120, 1024], P(None, 'gy', None, 'gx')
- regridded_zonal: float32 [64, 120, 1024], P('gy', None, 'gx')
- regridded_meridional: float32 [64, 120, 1024], P('gy', None, 'gx')
- adjusted_warmth: float32 [64, 120, 1024], P('gy', None, 'gx')
The draws below stay inside these ranges and needn't reach their ends.
Inputs may be any that keep to these rules, and one draw needn't show every extreme that they name: Target layer k draws on source layers leading_donor_level and leading_donor_level + 1, and leading_donor_level lies within 2 of k.
All inputs are finite; a program needn't handle non-finite values.
Results may differ from the reference program's by a relative error of at most 0.0003.
Values sent between devices are 32-bit elements; how exact they have to be, the bound alone decides.
No kernel may reach another device: no remote copies, remote signals or barrier semaphores. Data moves between devices by JAX's collectives and lax.ppermute only.
A program may use at most 64 MiB of HBM per device.

```python
import math
import jax
import jax.numpy as jnp
from jax import lax

NTR = 8
LEVEL_NUMBER = 120
EASTWARD_CELLS = 1024
NORTHWARD_CELLS = 64


def draw_leading_donor_level(key, part):
    offset = jax.random.randint(key, (NORTHWARD_CELLS, LEVEL_NUMBER, EASTWARD_CELLS), -2, 3, dtype=jnp.int32)
    layer_index = jnp.arange(LEVEL_NUMBER, dtype=jnp.int32)[None, :, None]
    return jnp.clip(layer_index + offset, 0, LEVEL_NUMBER - 2).astype(jnp.int32)


def steps_of(key, shape, cuts, least, largest):
    level = 1.0
    for position, shards_of in cuts:
        steps = jax.random.uniform(jax.random.fold_in(jax.random.fold_in(key, 6), position), (shards_of,), jnp.float32, least / len(cuts), largest / len(cuts))
        level = level * jnp.repeat(jnp.exp(steps), shape[position] // shards_of).reshape((-1,) + (1,) * (len(shape) - 1 - position))
    return level


def bell_draw(own_key, shape, width, limit, pieces=(), kind=jnp.bfloat16):
    values = jax.random.normal(own_key, shape, jnp.float32) * width
    if len(pieces) > 0:
        values = steps_of(own_key, shape, pieces, -0.22, 0.18) * values
    return jnp.clip(values, min=-limit, max=limit).astype(kind)


def setup_inputs(seed: int = 0) -> dict:
    arg_keys = jax.random.split(jax.random.key(seed), 9)
    return {
        "species_means": jnp.clip(jnp.exp(math.log(5.0) - 3.2227897 * jax.random.uniform(arg_keys[0], (NTR, NORTHWARD_CELLS, LEVEL_NUMBER, EASTWARD_CELLS), jnp.float32) ** steps_of(arg_keys[0], (NTR, NORTHWARD_CELLS, LEVEL_NUMBER, EASTWARD_CELLS), ((1, 32), (3, 8)), -0.2, 0.2)), 0.19921875, 5.0).astype(jnp.bfloat16),
        "zonal_edge_velocity": bell_draw(arg_keys[1], (NORTHWARD_CELLS, LEVEL_NUMBER, EASTWARD_CELLS), 1.0, 6.0, ((0, 32), (2, 8)), jnp.float32),
        "meridional_edge_velocity": bell_draw(arg_keys[2], (NORTHWARD_CELLS, LEVEL_NUMBER, EASTWARD_CELLS), 1.0, 6.0, ((0, 32), (2, 8)), jnp.float32),
        "scaled_warmth": jnp.clip(jnp.exp(math.log(2.0) - 1.3862944 * jax.random.uniform(arg_keys[3], (NORTHWARD_CELLS, LEVEL_NUMBER, EASTWARD_CELLS), jnp.float32) ** steps_of(arg_keys[3], (NORTHWARD_CELLS, LEVEL_NUMBER, EASTWARD_CELLS), ((0, 32), (2, 8)), -0.2, 0.2)), 0.5, 2.0),
        "donor_depths": jnp.clip(jnp.exp(math.log(2.0) - 1.3862944 * jax.random.uniform(arg_keys[4], (NORTHWARD_CELLS, LEVEL_NUMBER, EASTWARD_CELLS), jnp.float32) ** steps_of(arg_keys[4], (NORTHWARD_CELLS, LEVEL_NUMBER, EASTWARD_CELLS), ((0, 32), (2, 8)), -0.2, 0.2)), 0.5, 2.0),
        "leading_donor_level": draw_leading_donor_level(jax.random.fold_in(arg_keys[8], 71), 0),
        "opening_share": jnp.clip(0.44921875 * jax.random.uniform(arg_keys[6], (NORTHWARD_CELLS, LEVEL_NUMBER, EASTWARD_CELLS), jnp.float32) ** steps_of(arg_keys[6], (NORTHWARD_CELLS, LEVEL_NUMBER, EASTWARD_CELLS), ((0, 32), (2, 8)), -0.2, 0.2), 0.0, 0.44921875).astype(jnp.bfloat16),
        "closing_share": jnp.clip(0.546875 + 0.453125 * jax.random.uniform(arg_keys[7], (NORTHWARD_CELLS, LEVEL_NUMBER, EASTWARD_CELLS), jnp.float32) ** steps_of(arg_keys[7], (NORTHWARD_CELLS, LEVEL_NUMBER, EASTWARD_CELLS), ((0, 32), (2, 8)), -0.2, 0.2), 0.546875, 1.0).astype(jnp.bfloat16),
    }


thermal_rescale_factor = 3.5


def ppm_parts(values):
    layers = values.shape[-2]
    top_edge = 1.5 * values[..., 0:1, :] - 0.5 * values[..., 1:2, :]
    second_edge = 0.5 * (values[..., 0:1, :] + values[..., 1:2, :])
    inner_edge = (7.0 / 12.0) * (values[..., 1:layers - 2, :] + values[..., 2:layers - 1, :]) - (1.0 / 12.0) * (values[..., 0:layers - 3, :] + values[..., 3:layers, :])
    lower_edge = 0.5 * (values[..., layers - 2:layers - 1, :] + values[..., layers - 1:layers, :])
    bottom_edge = 1.5 * values[..., layers - 1:layers, :] - 0.5 * values[..., layers - 2:layers - 1, :]
    edge_values = jnp.concatenate([top_edge, second_edge, inner_edge, lower_edge, bottom_edge], axis=-2)
    left_edge = edge_values[..., :layers, :]
    right_edge = edge_values[..., 1:, :]
    return left_edge, right_edge - left_edge, 6.0 * values - 3.0 * (left_edge + right_edge)


def build_operator(donor_depths, leading_donor_level, opening_share, closing_share):
    start_frac = opening_share.astype(jnp.float32)
    end_frac = closing_share.astype(jnp.float32)
    next_layer = leading_donor_level + 1
    weight_first = (1.0 - start_frac) * jnp.take_along_axis(donor_depths, leading_donor_level, axis=-2)
    weight_second = end_frac * jnp.take_along_axis(donor_depths, next_layer, axis=-2)
    linear_first = 0.5 * (start_frac + 1.0)
    square_first = linear_first - (start_frac * start_frac + start_frac + 1.0) / 3.0
    linear_second = 0.5 * end_frac
    square_second = linear_second - end_frac * end_frac / 3.0
    return (leading_donor_level, next_layer, weight_first, weight_second, linear_first, square_first, linear_second, square_second)


def multiply_by_regrid_operator(operator, values):
    leading_donor_level, next_layer, weight_first, weight_second, linear_first, square_first, linear_second, square_second = operator
    left_edge, edge_slope, curvature = ppm_parts(values)
    first_index = jnp.broadcast_to(leading_donor_level, values.shape)
    second_index = jnp.broadcast_to(next_layer, values.shape)
    mean_first = jnp.take_along_axis(left_edge, first_index, axis=-2) + jnp.take_along_axis(edge_slope, first_index, axis=-2) * linear_first + jnp.take_along_axis(curvature, first_index, axis=-2) * square_first
    mean_second = jnp.take_along_axis(left_edge, second_index, axis=-2) + jnp.take_along_axis(edge_slope, second_index, axis=-2) * linear_second + jnp.take_along_axis(curvature, second_index, axis=-2) * square_second
    return (weight_first * mean_first + weight_second * mean_second) / (weight_first + weight_second)


def reference(species_means, zonal_edge_velocity, meridional_edge_velocity, scaled_warmth, donor_depths, leading_donor_level, opening_share, closing_share):
    vertical_regrid_operator = build_operator(donor_depths, leading_donor_level, opening_share, closing_share)
    north_op = build_operator(jnp.roll(donor_depths, -1, axis=0), jnp.roll(leading_donor_level, -1, axis=0), jnp.roll(opening_share, -1, axis=0), jnp.roll(closing_share, -1, axis=0))
    east_op = build_operator(jnp.roll(donor_depths, -1, axis=2), jnp.roll(leading_donor_level, -1, axis=2), jnp.roll(opening_share, -1, axis=2), jnp.roll(closing_share, -1, axis=2))
    regridded_depths = vertical_regrid_operator[2] + vertical_regrid_operator[3]
    tracer_new = lax.map(lambda tracer_field: multiply_by_regrid_operator(vertical_regrid_operator, tracer_field.astype(jnp.float32)), species_means)
    regridded_warmth = multiply_by_regrid_operator(vertical_regrid_operator, scaled_warmth)
    regridded_zonal = 0.5 * (multiply_by_regrid_operator(vertical_regrid_operator, zonal_edge_velocity) + multiply_by_regrid_operator(north_op, zonal_edge_velocity))
    regridded_meridional = 0.5 * (multiply_by_regrid_operator(vertical_regrid_operator, meridional_edge_velocity) + multiply_by_regrid_operator(east_op, meridional_edge_velocity))
    mass_before = lax.map(lambda tracer_field: jnp.sum(tracer_field.astype(jnp.float32) * donor_depths), species_means)
    mass_after = lax.map(lambda tracer_field: jnp.sum(tracer_field * regridded_depths), tracer_new)
    aggregate_regridded = jnp.sum(regridded_depths)
    preceding_zonal_aggregates = 0.5 * (donor_depths + jnp.roll(donor_depths, -1, axis=0))
    preceding_meridional_aggregates = 0.5 * (donor_depths + jnp.roll(donor_depths, -1, axis=2))
    zonal_edge_following = 0.5 * (regridded_depths + jnp.roll(regridded_depths, -1, axis=0))
    meridional_edge_following = 0.5 * (regridded_depths + jnp.roll(regridded_depths, -1, axis=2))
    preceding_enthalpy = thermal_rescale_factor * jnp.sum(donor_depths * scaled_warmth) + 0.5 * jnp.sum(preceding_zonal_aggregates * zonal_edge_velocity * zonal_edge_velocity) + 0.5 * jnp.sum(preceding_meridional_aggregates * meridional_edge_velocity * meridional_edge_velocity)
    kinetic_thermal_following = thermal_rescale_factor * jnp.sum(regridded_depths * regridded_warmth) + 0.5 * jnp.sum(zonal_edge_following * regridded_zonal * regridded_zonal) + 0.5 * jnp.sum(meridional_edge_following * regridded_meridional * regridded_meridional)
    tracers_out = tracer_new + ((mass_before - mass_after) / aggregate_regridded)[:, None, None, None]
    adjusted_warmth = regridded_warmth + (preceding_enthalpy - kinetic_thermal_following) / (thermal_rescale_factor * aggregate_regridded)
    return tracers_out, regridded_zonal, regridded_meridional, adjusted_warmth
```

```python
import functools

import jax
import jax.numpy as jnp
from jax import lax
from jax.experimental import pallas as pl
from jax.experimental.pallas import tpu as pltpu
from jax.sharding import PartitionSpec as P

HEAT = 3.5
PAD = 8
STEP = 8
DIAGONALS = tuple(range(-4, 6))
C7 = 7.0 / 12.0
C1 = 1.0 / 12.0


def block_of(k):
    return pl.ds(pl.multiple_of(k * STEP, STEP), STEP)


def padded_block(k):
    return pl.ds(pl.multiple_of(k * STEP + PAD, STEP), STEP)


def shifted(ref, k, *lead):
    return lambda d: ref[(*lead, pl.ds(k * STEP + (PAD + d), STEP), slice(None))]


def clear_pads(ref, layers):
    lead = ref.shape[:-2]
    zero = jnp.zeros(lead + (PAD, ref.shape[-1]), ref.dtype)
    every = (slice(None),) * len(lead)
    ref[(*every, pl.ds(0, PAD), slice(None))] = zero
    ref[(*every, pl.ds(PAD + layers, PAD), slice(None))] = zero


def pick(masks, values):
    chosen = values[-1]
    for mask, value in zip(masks[-2::-1], values[-2::-1]):
        chosen = jnp.where(mask, value, chosen)
    return chosen


def operator(depth, level, start, end, k, layers):
    offset = level - (lax.broadcasted_iota(jnp.int32, level.shape, 0) + k * STEP)
    masks = [offset == o for o in (-2, -1, 0, 1, 2)]
    depths = [depth(d) for d in range(-2, 4)]
    weight_first = (1.0 - start) * pick(masks, depths[0:5])
    weight_second = end * pick(masks, depths[1:6])
    thick = weight_first + weight_second
    inverse = 1.0 / thick
    first = weight_first * inverse
    second = weight_second * inverse
    linear_first = 0.5 * (start + 1.0)
    square_first = linear_first - (start * start + start + 1.0) * (1.0 / 3.0)
    linear_second = 0.5 * end
    square_second = linear_second - end * end * (1.0 / 3.0)
    triple_first = 3.0 * square_first
    triple_second = 3.0 * square_second
    edge0 = first * (1.0 - linear_first - triple_first)
    edge1 = first * (linear_first - triple_first) + second * (
        1.0 - linear_second - triple_second
    )
    edge2 = second * (linear_second - triple_second)
    mean0 = first * (2.0 * triple_first)
    mean1 = second * (2.0 * triple_second)
    top, under_top = level == 0, level == 1
    bottom, over_bottom = level == layers - 2, level == layers - 3
    e0 = (
        jnp.where(top | under_top, 0.0, -C1),
        jnp.where(top, 0.0, jnp.where(under_top, 0.5, C7)),
        jnp.where(top, 1.5, jnp.where(under_top, 0.5, C7)),
        jnp.where(top, -0.5, jnp.where(under_top, 0.0, -C1)),
    )
    outer = jnp.where(top | bottom, 0.0, -C1)
    inner = jnp.where(top | bottom, 0.5, C7)
    e2 = (
        jnp.where(bottom, -0.5, jnp.where(over_bottom, 0.0, -C1)),
        jnp.where(bottom, 1.5, jnp.where(over_bottom, 0.5, C7)),
        jnp.where(bottom, 0.0, jnp.where(over_bottom, 0.5, C7)),
        jnp.where(bottom | over_bottom, 0.0, -C1),
    )
    taps = {
        -2: e0[0] * edge0,
        -1: e0[1] * edge0 + outer * edge1,
        0: e0[2] * edge0 + inner * edge1 + e2[0] * edge2 + mean0,
        1: e0[3] * edge0 + inner * edge1 + e2[1] * edge2 + mean1,
        2: outer * edge1 + e2[2] * edge2,
        3: e2[3] * edge2,
    }
    diagonals = []
    for d in DIAGONALS:
        value = jnp.zeros_like(thick)
        for mask, o in zip(masks, (-2, -1, 0, 1, 2)):
            if d - o in taps:
                value = jnp.where(mask, taps[d - o], value)
        diagonals.append(value)
    return thick, diagonals


def apply_operator(diagonals, values):
    total = None
    for d, weight in zip(DIAGONALS, diagonals):
        term = weight * values(d)
        total = term if total is None else total + term
    return total


def pack_body(depth_ref, level_ref, start_ref, end_ref, row_ref, column_ref):
    layers = depth_ref.shape[1]
    rows = depth_ref.shape[0]

    def step(k, carry):
        block = block_of(k)
        lane = lax.broadcasted_iota(jnp.int32, (STEP, 128), 1)
        packed = jnp.zeros((STEP, 128), jnp.float32)
        for i, ref in enumerate((depth_ref, level_ref, start_ref, end_ref)):
            for r in range(rows):
                value = ref[r, block, :].astype(jnp.float32)
                if r == 0:
                    row_ref[i, block, :] = value
                target = i * rows + r
                if target:
                    value = pltpu.roll(value, target, 1)
                packed = jnp.where(lane == target, value, packed)
        column_ref[block, :] = packed
        return carry

    lax.fori_loop(0, layers // STEP, step, 0)


def sums_body(
    species_ref,
    zonal_ref,
    merid_ref,
    warmth_ref,
    depth_ref,
    level_ref,
    start_ref,
    end_ref,
    row_ref,
    column_ref,
    zonal_out,
    merid_out,
    sums_out,
    depth_pad,
    zonal_pad,
    merid_pad,
    west_pad,
    last_pad,
    adjoint_pad,
    thick_s,
    across_s,
    cross_s,
):
    tracers = species_ref.shape[0]
    rows, layers, _ = depth_ref.shape
    blocks = layers // STEP
    north, east = rows, rows + 1
    for ref in (depth_pad, zonal_pad, merid_pad, west_pad, last_pad, adjoint_pad):
        clear_pads(ref, layers)
    lane = lax.broadcasted_iota(jnp.int32, (STEP, 128), 1)

    def spread(k, carry):
        block, target = block_of(k), padded_block(k)
        last = jnp.zeros((STEP, 128), jnp.float32)
        for r in range(rows):
            depth_pad[r, target, :] = depth_ref[r, block, :]
            zonal_pad[r, target, :] = zonal_ref[r, block, :]
            value = merid_ref[r, block, :]
            merid_pad[r, target, :] = value
            west_pad[r, target, :] = pltpu.roll(value, 1, 1)
            last = jnp.where(lane == r, pltpu.roll(value, r + 1, 1), last)
        last_pad[target, :] = last
        depth_pad[north, target, :] = row_ref[0, block, :]
        depth_pad[east, target, :] = column_ref[block, :]
        return carry

    lax.fori_loop(0, blocks, spread, 0)

    def halo(k, carry):
        block = block_of(k)
        thick, diagonals = operator(
            shifted(depth_pad, k, north),
            row_ref[1, block, :].astype(jnp.int32),
            row_ref[2, block, :],
            row_ref[3, block, :],
            k,
            layers,
        )
        thick_s[north, block, :] = thick
        cross_s[rows - 1, block, :] = apply_operator(
            diagonals, shifted(zonal_pad, k, rows - 1)
        )
        packed = column_ref[block, :]
        thick, diagonals = operator(
            shifted(depth_pad, k, east),
            pltpu.roll(packed, 128 - rows, 1).astype(jnp.int32),
            pltpu.roll(packed, 128 - 2 * rows, 1),
            pltpu.roll(packed, 128 - 3 * rows, 1),
            k,
            layers,
        )
        thick_s[east, block, :] = thick
        across_s[rows, block, :] = apply_operator(diagonals, shifted(last_pad, k))
        return carry

    lax.fori_loop(0, blocks, halo, 0)

    def own(k, carry):
        block, target = block_of(k), padded_block(k)
        for r in range(rows):
            thick, diagonals = operator(
                shifted(depth_pad, k, r),
                level_ref[r, block, :],
                start_ref[r, block, :].astype(jnp.float32),
                end_ref[r, block, :].astype(jnp.float32),
                k,
                layers,
            )
            thick_s[r, block, :] = thick
            zonal_out[r, block, :] = apply_operator(diagonals, shifted(zonal_pad, k, r))
            merid_out[r, block, :] = apply_operator(diagonals, shifted(merid_pad, k, r))
            across_s[r, block, :] = apply_operator(diagonals, shifted(west_pad, k, r))
            if r:
                cross_s[r - 1, block, :] = apply_operator(
                    diagonals, shifted(zonal_pad, k, r - 1)
                )
            for i, weight in enumerate(diagonals):
                adjoint_pad[r, i, target, :] = thick * weight
        return carry

    lax.fori_loop(0, blocks, own, 0)

    def totals(k, carry):
        block = block_of(k)
        masses, energy, total = list(carry[:-2]), carry[-2], carry[-1]
        for r in range(rows):
            depth = depth_ref[r, block, :]
            back = None
            for i, d in enumerate(DIAGONALS):
                term = adjoint_pad[r, i, pl.ds(k * STEP + (PAD - d), STEP), :]
                back = term if back is None else back + term
            lost = depth - back
            for t in range(tracers):
                masses[t] = masses[t] + species_ref[t, r, block, :].astype(jnp.float32) * lost
            energy = energy + HEAT * (warmth_ref[r, block, :] * lost)
            thick = thick_s[r, block, :]
            total = total + thick
            zonal = 0.5 * (zonal_out[r, block, :] + cross_s[r, block, :])
            zonal_out[r, block, :] = zonal
            wind = zonal_ref[r, block, :]
            depth_next = depth_ref[r + 1, block, :] if r + 1 < rows else row_ref[0, block, :]
            thick_next = thick_s[r + 1, block, :]
            energy = energy + 0.25 * (
                (depth + depth_next) * (wind * wind) - (thick + thick_next) * (zonal * zonal)
            )

            def eastward(own_value, edge_value):
                return jnp.where(
                    lane == 127,
                    pltpu.roll(edge_value, 127 - r, 1),
                    pltpu.roll(own_value, 127, 1),
                )

            merid = 0.5 * (
                merid_out[r, block, :]
                + eastward(across_s[r, block, :], across_s[rows, block, :])
            )
            merid_out[r, block, :] = merid
            wind = merid_ref[r, block, :]
            depth_next = eastward(depth, column_ref[block, :])
            thick_next = eastward(thick, thick_s[east, block, :])
            energy = energy + 0.25 * (
                (depth + depth_next) * (wind * wind) - (thick + thick_next) * (merid * merid)
            )
        return (*masses, energy, total)

    zero = jnp.zeros((STEP, 128), jnp.float32)
    parts = lax.fori_loop(0, blocks, totals, (zero,) * (tracers + 2))
    row = jnp.zeros((STEP, 128), jnp.float32)
    for i, part in enumerate(parts):
        row = jnp.where(lane == i, jnp.sum(part, axis=1, keepdims=True), row)
    row = jnp.sum(row, axis=0, keepdims=True)
    sums_out[...] = jnp.broadcast_to(row, sums_out.shape)


def remap_body(
    species_ref,
    warmth_ref,
    depth_ref,
    level_ref,
    start_ref,
    end_ref,
    tracers_out,
    warmth_out,
    depth_pad,
    field_pad,
):
    tracers = species_ref.shape[0]
    rows, layers, _ = depth_ref.shape
    blocks = layers // STEP
    clear_pads(depth_pad, layers)
    clear_pads(field_pad, layers)

    def spread(k, carry):
        block, target = block_of(k), padded_block(k)
        for r in range(rows):
            depth_pad[r, target, :] = depth_ref[r, block, :]
            field_pad[tracers, r, target, :] = warmth_ref[r, block, :]
            for t in range(tracers):
                field_pad[t, r, target, :] = species_ref[t, r, block, :].astype(jnp.float32)
        return carry

    lax.fori_loop(0, blocks, spread, 0)

    def own(k, carry):
        block = block_of(k)
        for r in range(rows):
            _, diagonals = operator(
                shifted(depth_pad, k, r),
                level_ref[r, block, :],
                start_ref[r, block, :].astype(jnp.float32),
                end_ref[r, block, :].astype(jnp.float32),
                k,
                layers,
            )
            for t in range(tracers):
                tracers_out[t, r, block, :] = apply_operator(
                    diagonals, shifted(field_pad, k, t, r)
                )
            warmth_out[r, block, :] = apply_operator(
                diagonals, shifted(field_pad, k, tracers, r)
            )
        return carry

    lax.fori_loop(0, blocks, own, 0)


def ring_shift(value, axis, steps):
    count = lax.axis_size(axis)
    return lax.ppermute(value, axis, [(i, (i + steps) % count) for i in range(count)])


def cost(flops, moved):
    return pl.CostEstimate(flops=flops, bytes_accessed=moved, transcendentals=0)


def local(
    species,
    zonal,
    merid,
    warmth,
    depth,
    level,
    start,
    end,
):
    tracers = species.shape[0]
    rows, layers, columns = depth.shape
    devices = lax.axis_size(("gx", "gy"))
    f32 = functools.partial(jax.ShapeDtypeStruct, dtype=jnp.float32)
    vmem = pl.BlockSpec(memory_space=pltpu.VMEM)
    plane = (rows, layers, columns)
    tall = layers + 2 * PAD
    row_halo, column_halo = pl.pallas_call(
        pack_body,
        out_shape=(f32((4, layers, columns)), f32((layers, columns))),
        in_specs=[vmem] * 4,
        out_specs=(vmem, vmem),
        cost_estimate=cost(100_000, 600_000),
        name="pack_halo",
    )(depth, level, start, end)
    column_halo = ring_shift(column_halo, "gx", -1)
    row_halo = ring_shift(row_halo, "gy", -1)
    zonal_new, merid_new, sums = pl.pallas_call(
        sums_body,
        out_shape=(f32(plane), f32(plane), f32((devices, 128))),
        in_specs=[vmem] * 10,
        out_specs=(vmem,) * 3,
        scratch_shapes=[
            pltpu.VMEM((rows + 2, tall, columns), jnp.float32),
            pltpu.VMEM((rows, tall, columns), jnp.float32),
            pltpu.VMEM((rows, tall, columns), jnp.float32),
            pltpu.VMEM((rows, tall, columns), jnp.float32),
            pltpu.VMEM((tall, columns), jnp.float32),
            pltpu.VMEM((rows, len(DIAGONALS), tall, columns), jnp.float32),
            pltpu.VMEM((rows + 2, layers, columns), jnp.float32),
            pltpu.VMEM((rows + 1, layers, columns), jnp.float32),
            pltpu.VMEM((rows, layers, columns), jnp.float32),
        ],
        cost_estimate=cost(20_000_000, 2_000_000),
        name="wind_and_sums",
    )(species, zonal, merid, warmth, depth, level, start, end, row_halo, column_halo)
    gathered = lax.all_to_all(
        sums.reshape(devices, 1, 128), ("gx", "gy"), 0, 0, tiled=True
    )
    tracer_new, warmth_new = pl.pallas_call(
        remap_body,
        out_shape=(f32((tracers, *plane)), f32(plane)),
        in_specs=[vmem] * 6,
        out_specs=(vmem,) * 2,
        scratch_shapes=[
            pltpu.VMEM((rows, tall, columns), jnp.float32),
            pltpu.VMEM((tracers + 1, rows, tall, columns), jnp.float32),
        ],
        cost_estimate=cost(20_000_000, 2_000_000),
        name="tracer_remap",
    )(species, warmth, depth, level, start, end)
    totals = jnp.sum(gathered, axis=(0, 1))
    total = totals[tracers + 1]
    tracers_out = tracer_new + (totals[:tracers] / total)[:, None, None, None]
    warmth_out = warmth_new + totals[tracers] / (HEAT * total)
    return tracers_out, zonal_new, merid_new, warmth_out


def solution(mesh):
    plane = P("gy", None, "gx")
    stack = P(None, "gy", None, "gx")
    return jax.shard_map(
        local,
        mesh=mesh,
        in_specs=(stack,) + (plane,) * 7,
        out_specs=(stack, plane, plane, plane),
        check_vma=False,
    )
```

```python
import functools

import jax
import jax.numpy as jnp
from jax import lax
from jax.experimental import pallas as pl
from jax.experimental.pallas import tpu as pltpu
from jax.sharding import PartitionSpec as P

HEAT = 3.5
PAD = 8
STEP = 8
DIAGONALS = tuple(range(-4, 6))
C7 = 7.0 / 12.0
C1 = 1.0 / 12.0


def block_of(k):
    return pl.ds(pl.multiple_of(k * STEP, STEP), STEP)


def padded_block(k):
    return pl.ds(pl.multiple_of(k * STEP + PAD, STEP), STEP)


def shifted(ref, k, *lead):
    return lambda d: ref[(*lead, pl.ds(k * STEP + (PAD + d), STEP), slice(None))]


def layers_of(k):
    return lax.broadcasted_iota(jnp.int32, (STEP, 128), 0) + k * STEP


def clear_pads(ref, layers):
    lead = ref.shape[:-2]
    zero = jnp.zeros(lead + (PAD, ref.shape[-1]), ref.dtype)
    every = (slice(None),) * len(lead)
    ref[(*every, pl.ds(0, PAD), slice(None))] = zero
    ref[(*every, pl.ds(PAD + layers, PAD), slice(None))] = zero


def pick(masks, values):
    chosen = values[-1]
    for mask, value in zip(masks[-2::-1], values[-2::-1]):
        chosen = jnp.where(mask, value, chosen)
    return chosen


def operator(depth, level, start, end, target, layers):
    offset = level - target
    masks = [offset == o for o in (-2, -1, 0, 1, 2)]
    depths = [depth(d) for d in range(-2, 4)]
    weight_first = (1.0 - start) * pick(masks, depths[0:5])
    weight_second = end * pick(masks, depths[1:6])
    thick = weight_first + weight_second
    inverse = 1.0 / thick
    first = weight_first * inverse
    second = weight_second * inverse
    linear_first = 0.5 * (start + 1.0)
    square_first = linear_first - (start * start + start + 1.0) * (1.0 / 3.0)
    linear_second = 0.5 * end
    square_second = linear_second - end * end * (1.0 / 3.0)
    triple_first = 3.0 * square_first
    triple_second = 3.0 * square_second
    edge0 = first * (1.0 - linear_first - triple_first)
    edge1 = first * (linear_first - triple_first) + second * (
        1.0 - linear_second - triple_second
    )
    edge2 = second * (linear_second - triple_second)
    mean0 = first * (2.0 * triple_first)
    mean1 = second * (2.0 * triple_second)
    top, under_top = level == 0, level == 1
    bottom, over_bottom = level == layers - 2, level == layers - 3
    e0 = (
        jnp.where(top | under_top, 0.0, -C1),
        jnp.where(top, 0.0, jnp.where(under_top, 0.5, C7)),
        jnp.where(top, 1.5, jnp.where(under_top, 0.5, C7)),
        jnp.where(top, -0.5, jnp.where(under_top, 0.0, -C1)),
    )
    outer = jnp.where(top | bottom, 0.0, -C1)
    inner = jnp.where(top | bottom, 0.5, C7)
    e2 = (
        jnp.where(bottom, -0.5, jnp.where(over_bottom, 0.0, -C1)),
        jnp.where(bottom, 1.5, jnp.where(over_bottom, 0.5, C7)),
        jnp.where(bottom, 0.0, jnp.where(over_bottom, 0.5, C7)),
        jnp.where(bottom | over_bottom, 0.0, -C1),
    )
    taps = {
        -2: e0[0] * edge0,
        -1: e0[1] * edge0 + outer * edge1,
        0: e0[2] * edge0 + inner * edge1 + e2[0] * edge2 + mean0,
        1: e0[3] * edge0 + inner * edge1 + e2[1] * edge2 + mean1,
        2: outer * edge1 + e2[2] * edge2,
        3: e2[3] * edge2,
    }
    diagonals = []
    for d in DIAGONALS:
        value = jnp.zeros_like(thick)
        for mask, o in zip(masks, (-2, -1, 0, 1, 2)):
            if d - o in taps:
                value = jnp.where(mask, taps[d - o], value)
        diagonals.append(value)
    return thick, diagonals


def apply_operator(diagonals, values):
    total = None
    for d, weight in zip(DIAGONALS, diagonals):
        term = weight * values(d)
        total = term if total is None else total + term
    return total


def pack_body(
    depth_ref, level_ref, start_ref, end_ref, merid_ref, row_ref, send_ref, keep_ref, columns_s
):
    rows, layers, _ = depth_ref.shape
    lane = lax.broadcasted_iota(jnp.int32, (STEP, 128), 1)

    def step(k, carry):
        block = block_of(k)
        packed = jnp.zeros((STEP, 128), jnp.float32)
        for i, ref in enumerate((depth_ref, level_ref, start_ref, end_ref)):
            for r in range(rows):
                value = ref[r, block, :].astype(jnp.float32)
                if r == 0:
                    row_ref[i, block, :] = value
                place = i * rows + r
                if place:
                    value = pltpu.roll(value, place, 1)
                packed = jnp.where(lane == place, value, packed)
        for i, ref in enumerate((merid_ref, depth_ref)):
            for r in range(rows):
                place = STEP + i * rows + r
                packed = jnp.where(lane == place, pltpu.roll(ref[r, block, :], place + 1, 1), packed)
        columns_s[block, :] = packed
        return carry

    lax.fori_loop(0, layers // STEP, step, 0)
    columns_s[pl.ds(layers, 128 - layers), :] = jnp.zeros((128 - layers, 128), jnp.float32)
    across = columns_s[...].T
    send_ref[...] = across[0:STEP]
    keep_ref[...] = across[STEP : 2 * STEP]


def own_body(
    species_ref,
    zonal_ref,
    merid_ref,
    warmth_ref,
    depth_ref,
    level_ref,
    start_ref,
    end_ref,
    zonal_out,
    merid_out,
    last_out,
    edge_out,
    sums_out,
    depth_pad,
    zonal_pad,
    merid_pad,
    west_pad,
    adjoint_pad,
    thick_s,
    across_s,
    cross_s,
    columns_s,
):
    tracers = species_ref.shape[0]
    rows, layers, _ = depth_ref.shape
    blocks = layers // STEP
    for ref in (depth_pad, zonal_pad, merid_pad, west_pad, adjoint_pad):
        clear_pads(ref, layers)
    lane = lax.broadcasted_iota(jnp.int32, (STEP, 128), 1)

    def spread(k, carry):
        block, target = block_of(k), padded_block(k)
        for r in range(rows):
            depth_pad[r, target, :] = depth_ref[r, block, :]
            zonal_pad[r, target, :] = zonal_ref[r, block, :]
            value = merid_ref[r, block, :]
            merid_pad[r, target, :] = value
            west_pad[r, target, :] = pltpu.roll(value, 1, 1)
        return carry

    lax.fori_loop(0, blocks, spread, 0)

    def own(k, carry):
        block, target = block_of(k), padded_block(k)
        columns = jnp.zeros((STEP, 128), jnp.float32)
        for r in range(rows):
            thick, diagonals = operator(
                shifted(depth_pad, k, r),
                level_ref[r, block, :],
                start_ref[r, block, :].astype(jnp.float32),
                end_ref[r, block, :].astype(jnp.float32),
                layers_of(k),
                layers,
            )
            thick_s[r, block, :] = thick
            zonal_out[r, block, :] = apply_operator(diagonals, shifted(zonal_pad, k, r))
            merid = apply_operator(diagonals, shifted(merid_pad, k, r))
            merid_out[r, block, :] = merid
            across_s[r, block, :] = apply_operator(diagonals, shifted(west_pad, k, r))
            if r:
                cross_s[r - 1, block, :] = apply_operator(
                    diagonals, shifted(zonal_pad, k, r - 1)
                )
            for i, weight in enumerate(diagonals):
                adjoint_pad[r, i, target, :] = thick * weight
            for i, value in enumerate((thick, merid)):
                place = i * rows + r
                columns = jnp.where(lane == place, pltpu.roll(value, place + 1, 1), columns)
        columns_s[block, :] = columns
        return carry

    lax.fori_loop(0, blocks, own, 0)
    columns_s[pl.ds(layers, 128 - layers), :] = jnp.zeros((128 - layers, 128), jnp.float32)
    edge_out[...] = columns_s[...].T[0:STEP]

    def totals(k, carry):
        block = block_of(k)
        masses, energy, total = list(carry[:-2]), carry[-2], carry[-1]
        for r in range(rows):
            depth = depth_ref[r, block, :]
            back = None
            for i, d in enumerate(DIAGONALS):
                term = adjoint_pad[r, i, pl.ds(k * STEP + (PAD - d), STEP), :]
                back = term if back is None else back + term
            lost = depth - back
            for t in range(tracers):
                masses[t] = masses[t] + species_ref[t, r, block, :].astype(jnp.float32) * lost
            energy = energy + HEAT * (warmth_ref[r, block, :] * lost)
            thick = thick_s[r, block, :]
            total = total + thick
            if r + 1 < rows:
                zonal = 0.5 * (zonal_out[r, block, :] + cross_s[r, block, :])
                zonal_out[r, block, :] = zonal
                wind = zonal_ref[r, block, :]
                energy = energy + 0.25 * (
                    (depth + depth_ref[r + 1, block, :]) * (wind * wind)
                    - (thick + thick_s[r + 1, block, :]) * (zonal * zonal)
                )
            else:
                last_out[0, block, :] = zonal_ref[r, block, :]
                last_out[1, block, :] = depth
                last_out[2, block, :] = thick
            merid = 0.5 * (merid_out[r, block, :] + pltpu.roll(across_s[r, block, :], 127, 1))
            merid_out[r, block, :] = merid
            wind = merid_ref[r, block, :]
            kinetic = (depth + pltpu.roll(depth, 127, 1)) * (wind * wind) - (
                thick + pltpu.roll(thick, 127, 1)
            ) * (merid * merid)
            energy = energy + jnp.where(lane == 127, 0.0, 0.25 * kinetic)
        return (*masses, energy, total)

    zero = jnp.zeros((STEP, 128), jnp.float32)
    parts = lax.fori_loop(0, blocks, totals, (zero,) * (tracers + 2))
    for i, part in enumerate(parts):
        sums_out[i] = part


def halo_body(
    row_ref,
    column_ref,
    keep_ref,
    zonal_ref,
    last_ref,
    edge_ref,
    parts_ref,
    zonal_out,
    merid_out,
    sums_out,
    depth_pad,
    zonal_pad,
):
    layers = row_ref.shape[1]
    rows = zonal_ref.shape[0]
    blocks = layers // STEP
    clear_pads(depth_pad, layers)
    clear_pads(zonal_pad, layers)
    lane = lax.broadcasted_iota(jnp.int32, (STEP, 128), 1)
    sublane = lax.broadcasted_iota(jnp.int32, (STEP, 128), 0)

    packed = column_ref[...]
    thick, diagonals = operator(
        lambda d: pltpu.roll(packed, -d % 128, 1),
        pltpu.roll(packed, STEP - rows, 0).astype(jnp.int32),
        pltpu.roll(packed, STEP - 2 * rows, 0),
        pltpu.roll(packed, STEP - 3 * rows, 0),
        lane,
        layers,
    )
    wind = keep_ref[...]
    depth = pltpu.roll(wind, STEP - rows, 0)
    edge = edge_ref[...]
    merid = 0.5 * (
        pltpu.roll(edge, STEP - rows, 0)
        + apply_operator(diagonals, lambda d: pltpu.roll(wind, -d % 128, 1))
    )
    merid_out[...] = merid
    kinetic = (depth + packed) * (wind * wind) - (edge + thick) * (merid * merid)
    energy = jnp.where((lane < layers) & (sublane < rows), 0.25 * kinetic, 0.0)

    def spread(k, carry):
        block, target = block_of(k), padded_block(k)
        depth_pad[target, :] = row_ref[0, block, :]
        zonal_pad[target, :] = last_ref[0, block, :]
        return carry

    lax.fori_loop(0, blocks, spread, 0, unroll=5)

    def north(k, energy):
        block = block_of(k)
        thick, diagonals = operator(
            shifted(depth_pad, k),
            row_ref[1, block, :].astype(jnp.int32),
            row_ref[2, block, :],
            row_ref[3, block, :],
            layers_of(k),
            layers,
        )
        zonal = 0.5 * (
            zonal_ref[rows - 1, block, :] + apply_operator(diagonals, shifted(zonal_pad, k))
        )
        zonal_out[block, :] = zonal
        wind = last_ref[0, block, :]
        return energy + 0.25 * (
            (last_ref[1, block, :] + row_ref[0, block, :]) * (wind * wind)
            - (last_ref[2, block, :] + thick) * (zonal * zonal)
        )

    energy = lax.fori_loop(0, blocks, north, energy)
    row = jnp.zeros((STEP, 128), jnp.float32)
    count = parts_ref.shape[0]
    for i in range(count):
        part = parts_ref[i]
        if i == count - 2:
            part = part + energy
        row = jnp.where(lane == i, jnp.sum(part, axis=1, keepdims=True), row)
    row = jnp.sum(row, axis=0, keepdims=True)
    sums_out[...] = jnp.broadcast_to(row, sums_out.shape)


def remap_body(
    species_ref,
    warmth_ref,
    depth_ref,
    level_ref,
    start_ref,
    end_ref,
    zonal_ref,
    last_ref,
    merid_ref,
    edge_ref,
    tracers_out,
    warmth_out,
    zonal_out,
    merid_out,
    depth_pad,
    field_pad,
    columns_s,
):
    tracers = species_ref.shape[0]
    rows, layers, _ = depth_ref.shape
    blocks = layers // STEP
    clear_pads(depth_pad, layers)
    clear_pads(field_pad, layers)
    lane = lax.broadcasted_iota(jnp.int32, (STEP, 128), 1)
    columns_s[...] = jnp.zeros_like(columns_s)
    columns_s[0:STEP, :] = edge_ref[...]
    columns_s[...] = columns_s[...].T

    def spread(k, carry):
        block, target = block_of(k), padded_block(k)
        edge = columns_s[block, :]
        for r in range(rows):
            depth_pad[r, target, :] = depth_ref[r, block, :]
            field_pad[tracers, r, target, :] = warmth_ref[r, block, :]
            for t in range(tracers):
                field_pad[t, r, target, :] = species_ref[t, r, block, :].astype(jnp.float32)
            zonal_out[r, block, :] = (
                zonal_ref[r, block, :] if r + 1 < rows else last_ref[block, :]
            )
            merid_out[r, block, :] = jnp.where(
                lane == 127, pltpu.roll(edge, 127 - r, 1), merid_ref[r, block, :]
            )
        return carry

    lax.fori_loop(0, blocks, spread, 0)

    def own(k, carry):
        block = block_of(k)
        for r in range(rows):
            _, diagonals = operator(
                shifted(depth_pad, k, r),
                level_ref[r, block, :],
                start_ref[r, block, :].astype(jnp.float32),
                end_ref[r, block, :].astype(jnp.float32),
                layers_of(k),
                layers,
            )
            for t in range(tracers):
                tracers_out[t, r, block, :] = apply_operator(
                    diagonals, shifted(field_pad, k, t, r)
                )
            warmth_out[r, block, :] = apply_operator(
                diagonals, shifted(field_pad, k, tracers, r)
            )
        return carry

    lax.fori_loop(0, blocks, own, 0)


def correct_body(gathered_ref, tracer_ref, warmth_ref, tracers_out, warmth_out, new_s, heat_s, sem):
    tracers = tracer_ref.shape[0]
    totals = jnp.sum(gathered_ref[...], axis=0, keepdims=True)
    total = totals[:, tracers + 1 : tracers + 2]
    scale = 1.0 / total
    copies = []
    for t in range(tracers):
        new_s[t] = tracer_ref[t] + totals[:, t : t + 1] * scale
        copies.append(pltpu.make_async_copy(new_s.at[t], tracers_out.at[t], sem.at[t]))
        copies[-1].start()
    heat_s[...] = warmth_ref[...] + totals[:, tracers : tracers + 1] * (scale * (1.0 / HEAT))
    copies.append(pltpu.make_async_copy(heat_s, warmth_out, sem.at[tracers]))
    copies[-1].start()
    for copy in copies:
        copy.wait()


def ring_shift(value, axis, steps):
    count = lax.axis_size(axis)
    return lax.ppermute(value, axis, [(i, (i + steps) % count) for i in range(count)])


def kernel(body, name, flops, moved, scratch, near, outs, operands):
    operands = [
        pltpu.with_memory_space_constraint(x, pltpu.VMEM if i in near else pltpu.HBM)
        for i, x in enumerate(operands)
    ]
    vmem = pl.BlockSpec(memory_space=pltpu.VMEM)
    hbm = pl.BlockSpec(memory_space=pl.ANY)
    return pl.pallas_call(
        body,
        out_shape=tuple(
            pltpu.VMEM(shape, jnp.float32)
            if place == "vmem"
            else jax.ShapeDtypeStruct(shape, jnp.float32)
            for shape, place in outs
        ),
        in_specs=[vmem] * len(operands),
        out_specs=tuple(hbm if place == "any" else vmem for _, place in outs),
        scratch_shapes=scratch,
        cost_estimate=pl.CostEstimate(flops=flops, bytes_accessed=moved, transcendentals=0),
        compiler_params=pltpu.CompilerParams(vmem_limit_bytes=24 * 2**20),
        name=name,
    )(*operands)


def local(species, zonal, merid, warmth, depth, level, start, end):
    tracers = species.shape[0]
    plane = rows, layers, columns = depth.shape
    devices = lax.axis_size(("gx", "gy"))
    tall = layers + 2 * PAD
    tile = (STEP, 128)
    real = functools.partial(pltpu.VMEM, dtype=jnp.float32)
    row_halo, column_halo, keep = kernel(
        pack_body,
        "pack_halo",
        100_000,
        600_000,
        [real((128, 128))],
        (),
        [((4, layers, columns), "vmem"), (tile, "vmem"), (tile, "vmem")],
        (depth, level, start, end, merid),
    )
    row_halo = ring_shift(row_halo, "gy", -1)
    column_halo = ring_shift(column_halo, "gx", -1)
    zonal_part, merid_part, last, edge, parts = kernel(
        own_body,
        "own_columns",
        20_000_000,
        2_000_000,
        [
            real((rows, tall, columns)),
            real((rows, tall, columns)),
            real((rows, tall, columns)),
            real((rows, tall, columns)),
            real((rows, len(DIAGONALS), tall, columns)),
            real(plane),
            real(plane),
            real(plane),
            real((128, 128)),
        ],
        (),
        [
            (plane, "vmem"),
            (plane, "vmem"),
            ((3, layers, columns), "vmem"),
            (tile, "vmem"),
            ((tracers + 2, *tile), "vmem"),
        ],
        (species, zonal, merid, warmth, depth, level, start, end),
    )
    zonal_last, merid_last, sums = kernel(
        halo_body,
        "halo_faces",
        2_000_000,
        500_000,
        [real((tall, columns)), real((tall, columns))],
        range(7),
        [((layers, columns), "vmem"), (tile, "vmem"), ((devices, 128), "vmem")],
        (row_halo, column_halo, keep, zonal_part, last, edge, parts),
    )
    gathered = lax.all_to_all(sums.reshape(devices, 1, 128), ("gx", "gy"), 0, 0, tiled=True)
    tracer_new, warmth_new, zonal_new, merid_new = kernel(
        remap_body,
        "tracer_remap",
        20_000_000,
        2_000_000,
        [
            real((rows, tall, columns)),
            real((tracers + 1, rows, tall, columns)),
            real((128, 128)),
        ],
        range(6, 10),
        [((tracers, *plane), "vmem"), (plane, "vmem"), (plane, "hbm"), (plane, "hbm")],
        (species, warmth, depth, level, start, end, zonal_part, zonal_last, merid_part, merid_last),
    )
    tracers_out, warmth_out = kernel(
        correct_body,
        "corrections",
        1_000_000,
        2_000_000,
        [real((tracers, *plane)), real(plane), pltpu.SemaphoreType.DMA((tracers + 1,))],
        range(3),
        [((tracers, *plane), "any"), (plane, "any")],
        (gathered.reshape(devices, 128), tracer_new, warmth_new),
    )
    return tracers_out, zonal_new, merid_new, warmth_out


def solution(mesh):
    plane = P("gy", None, "gx")
    stack = P(None, "gy", None, "gx")
    return jax.shard_map(
        local,
        mesh=mesh,
        in_specs=(stack,) + (plane,) * 7,
        out_specs=(stack, plane, plane, plane),
        check_vma=False,
    )
```

```python
import functools

import jax
import jax.numpy as jnp
from jax import lax
from jax.experimental import pallas as pl
from jax.experimental.pallas import tpu as pltpu
from jax.sharding import PartitionSpec as P


HEAT = 3.5
PAD = 8
STEP = 8
DIAGONALS = tuple(range(-4, 6))
C7 = 7.0 / 12.0
C1 = 1.0 / 12.0


def block_of(k, first=0):
    start = k * STEP + first
    return pl.ds(start if isinstance(k, int) else pl.multiple_of(start, STEP), STEP)


def padded_block(k):
    return block_of(k, PAD)


def shifted(ref, k, *lead):
    return lambda d: ref[(*lead, pl.ds(k * STEP + (PAD + d), STEP), slice(None))]


def layers_of(k):
    return lax.broadcasted_iota(jnp.int32, (STEP, 128), 0) + k * STEP


def clear_pads(ref, layers):
    lead = ref.shape[:-2]
    zero = jnp.zeros(lead + (PAD, ref.shape[-1]), ref.dtype)
    every = (slice(None),) * len(lead)
    ref[(*every, pl.ds(0, PAD), slice(None))] = zero
    ref[(*every, pl.ds(PAD + layers, PAD), slice(None))] = zero


def pick(masks, values):
    chosen = values[-1]
    for mask, value in zip(masks[-2::-1], values[-2::-1]):
        chosen = jnp.where(mask, value, chosen)
    return chosen


def operator(depth, level, start, end, target, layers):
    offset = level - target
    masks = [offset == o for o in (-2, -1, 0, 1, 2)]
    depths = [depth(d) for d in range(-2, 4)]
    weight_first = (1.0 - start) * pick(masks, depths[0:5])
    weight_second = end * pick(masks, depths[1:6])
    thick = weight_first + weight_second
    inverse = 1.0 / thick
    first = weight_first * inverse
    second = weight_second * inverse
    linear_first = 0.5 * (start + 1.0)
    square_first = linear_first - (start * start + start + 1.0) * (1.0 / 3.0)
    linear_second = 0.5 * end
    square_second = linear_second - end * end * (1.0 / 3.0)
    triple_first = 3.0 * square_first
    triple_second = 3.0 * square_second
    edge0 = first * (1.0 - linear_first - triple_first)
    edge1 = first * (linear_first - triple_first) + second * (
        1.0 - linear_second - triple_second
    )
    edge2 = second * (linear_second - triple_second)
    mean0 = first * (2.0 * triple_first)
    mean1 = second * (2.0 * triple_second)
    top, under_top = level == 0, level == 1
    bottom, over_bottom = level == layers - 2, level == layers - 3
    e0 = (
        jnp.where(top | under_top, 0.0, -C1),
        jnp.where(top, 0.0, jnp.where(under_top, 0.5, C7)),
        jnp.where(top, 1.5, jnp.where(under_top, 0.5, C7)),
        jnp.where(top, -0.5, jnp.where(under_top, 0.0, -C1)),
    )
    outer = jnp.where(top | bottom, 0.0, -C1)
    inner = jnp.where(top | bottom, 0.5, C7)
    e2 = (
        jnp.where(bottom, -0.5, jnp.where(over_bottom, 0.0, -C1)),
        jnp.where(bottom, 1.5, jnp.where(over_bottom, 0.5, C7)),
        jnp.where(bottom, 0.0, jnp.where(over_bottom, 0.5, C7)),
        jnp.where(bottom | over_bottom, 0.0, -C1),
    )
    taps = {
        -2: e0[0] * edge0,
        -1: e0[1] * edge0 + outer * edge1,
        0: e0[2] * edge0 + inner * edge1 + e2[0] * edge2 + mean0,
        1: e0[3] * edge0 + inner * edge1 + e2[1] * edge2 + mean1,
        2: outer * edge1 + e2[2] * edge2,
        3: e2[3] * edge2,
    }
    diagonals = []
    for d in DIAGONALS:
        value = jnp.zeros_like(thick)
        for mask, o in zip(masks, (-2, -1, 0, 1, 2)):
            if d - o in taps:
                value = jnp.where(mask, taps[d - o], value)
        diagonals.append(value)
    return thick, diagonals


def apply_operator(diagonals, values):
    total = None
    for d, weight in zip(DIAGONALS, diagonals):
        term = weight * values(d)
        total = term if total is None else total + term
    return total


def pack_body(depth_ref, level_ref, start_ref, end_ref, row_ref, send_ref, columns_s):
    rows, layers, columns = depth_ref.shape
    lane = lax.broadcasted_iota(jnp.int32, (layers, columns), 1)
    packed = jnp.zeros((layers, columns), jnp.float32)
    for i, ref in enumerate((depth_ref, level_ref, start_ref, end_ref)):
        for r in range(rows):
            value = ref[r].astype(jnp.float32)
            if r == 0:
                row_ref[i] = value
            place = i * rows + r
            if place:
                value = pltpu.roll(value, place, 1)
            packed = jnp.where(lane == place, value, packed)
    columns_s[pl.ds(0, layers), :] = packed
    columns_s[pl.ds(layers, 128 - layers), :] = jnp.zeros((128 - layers, 128), jnp.float32)
    send_ref[...] = columns_s[...].T[0:STEP]


def own_body(
    species_ref,
    zonal_ref,
    merid_ref,
    warmth_ref,
    depth_ref,
    level_ref,
    start_ref,
    end_ref,
    tracers_out,
    warmth_out,
    zonal_out,
    merid_out,
    last_out,
    edge_out,
    sums_out,
    depth_pad,
    zonal_pad,
    merid_pad,
    west_pad,
    field_pad,
    thick_s,
    across_s,
    columns_s,
):
    tracers = species_ref.shape[0]
    rows, layers, _ = depth_ref.shape
    blocks = layers // STEP
    for ref in (depth_pad, zonal_pad, merid_pad, west_pad, field_pad):
        clear_pads(ref, layers)

    def spread(k, carry):
        block, target = block_of(k), padded_block(k)
        for r in range(rows):
            depth_pad[r, target, :] = depth_ref[r, block, :]
            zonal_pad[r, target, :] = zonal_ref[r, block, :]
            merid_pad[r, target, :] = merid_ref[r, block, :]
            field_pad[tracers, r, target, :] = warmth_ref[r, block, :]
            for t in range(tracers):
                field_pad[t, r, target, :] = species_ref[t, r, block, :].astype(jnp.float32)
        return carry

    lax.fori_loop(0, blocks, spread, 0)
    for r in range(rows):
        west_pad[r, pl.ds(PAD, layers), :] = pltpu.roll(merid_ref[r], 1, 1)

    def own(k, carry):
        block, target = block_of(k), padded_block(k)
        lost, energy, total = list(carry[:-2]), carry[-2], carry[-1]
        thick_before = zonal_before = None
        for r in range(rows):
            thick, diagonals = operator(
                shifted(depth_pad, k, r),
                level_ref[r, block, :],
                start_ref[r, block, :].astype(jnp.float32),
                end_ref[r, block, :].astype(jnp.float32),
                layers_of(k),
                layers,
            )
            depth = depth_ref[r, block, :]
            thick_s[r, block, :] = thick
            total = total + thick
            merid_out[r, block, :] = apply_operator(diagonals, shifted(merid_pad, k, r))
            across_s[r, block, :] = apply_operator(diagonals, shifted(west_pad, k, r))
            for t in range(tracers):
                new = apply_operator(diagonals, shifted(field_pad, k, t, r))
                tracers_out[t, r, block, :] = new
                lost[t] = lost[t] + (depth * field_pad[t, r, target, :] - thick * new)
            new = apply_operator(diagonals, shifted(field_pad, k, tracers, r))
            warmth_out[r, block, :] = new
            energy = energy + HEAT * (depth * field_pad[tracers, r, target, :] - thick * new)
            zonal = apply_operator(diagonals, shifted(zonal_pad, k, r))
            if r:
                crossed = 0.5 * (
                    zonal_before + apply_operator(diagonals, shifted(zonal_pad, k, r - 1))
                )
                zonal_out[r - 1, block, :] = crossed
                wind = zonal_ref[r - 1, block, :]
                energy = energy + 0.25 * (
                    (depth_ref[r - 1, block, :] + depth) * (wind * wind)
                    - (thick_before + thick) * (crossed * crossed)
                )
            if r + 1 == rows:
                zonal_out[r, block, :] = zonal
                last_out[0, block, :] = zonal_ref[r, block, :]
                last_out[1, block, :] = depth
                last_out[2, block, :] = thick
            thick_before, zonal_before = thick, zonal
        return (*lost, energy, total)

    zero = jnp.zeros((STEP, 128), jnp.float32)
    parts = lax.fori_loop(0, blocks, own, (zero,) * (tracers + 2))

    lane = lax.broadcasted_iota(jnp.int32, (layers, 128), 1)
    columns = jnp.zeros((layers, 128), jnp.float32)
    shared = jnp.zeros((STEP, 128), jnp.float32)
    for r in range(rows):
        for i, ref in enumerate((thick_s, merid_out, depth_ref, merid_ref)):
            place = i * rows + r
            columns = jnp.where(lane == place, pltpu.roll(ref[r], place + 1, 1), columns)
        depth, thick, wind = depth_ref[r], thick_s[r], merid_ref[r]
        merid = 0.5 * (merid_out[r] + pltpu.roll(across_s[r], 127, 1))
        merid_out[r] = merid
        kinetic = (depth + pltpu.roll(depth, 127, 1)) * (wind * wind) - (
            thick + pltpu.roll(thick, 127, 1)
        ) * (merid * merid)
        shared = shared + jnp.sum(kinetic.reshape(blocks, STEP, 128), axis=0)
    columns_s[pl.ds(0, layers), :] = columns
    columns_s[pl.ds(layers, 128 - layers), :] = jnp.zeros((128 - layers, 128), jnp.float32)
    edge_out[...] = columns_s[...].T[0:STEP]

    lane = lax.broadcasted_iota(jnp.int32, (STEP, 128), 1)
    row = jnp.zeros((STEP, 128), jnp.float32)
    for i, part in enumerate(parts):
        if i != tracers:
            row = jnp.where(lane == i, jnp.sum(part, axis=1, keepdims=True), row)
    sums_out[0] = row
    sums_out[1] = parts[tracers] + jnp.where(lane == 127, 0.0, 0.25 * shared)


def north_faces(row_ref, zonal_ref, last_ref, energy, zonal_out, depth_pad, zonal_pad):
    layers = row_ref.shape[1]
    rows = zonal_ref.shape[0]
    clear_pads(depth_pad, layers)
    clear_pads(zonal_pad, layers)
    depth_pad[pl.ds(PAD, layers), :] = row_ref[0]
    zonal_pad[pl.ds(PAD, layers), :] = last_ref[0]
    for k in range(layers // STEP):
        block = block_of(k)
        thick, diagonals = operator(
            shifted(depth_pad, k),
            row_ref[1, block, :].astype(jnp.int32),
            row_ref[2, block, :],
            row_ref[3, block, :],
            layers_of(k),
            layers,
        )
        zonal = 0.5 * (
            zonal_ref[rows - 1, block, :] + apply_operator(diagonals, shifted(zonal_pad, k))
        )
        zonal_out[block, :] = zonal
        wind = last_ref[0, block, :]
        energy = energy + 0.25 * (
            (last_ref[1, block, :] + row_ref[0, block, :]) * (wind * wind)
            - (last_ref[2, block, :] + thick) * (zonal * zonal)
        )
    return energy


def finish_sums(tracers, sums, energy, sums_out):
    lane = lax.broadcasted_iota(jnp.int32, (STEP, 128), 1)
    energy = jnp.sum(energy, axis=1, keepdims=True)
    row = jnp.sum(jnp.where(lane == tracers, energy, sums), axis=0, keepdims=True)
    sums_out[...] = jnp.broadcast_to(row, sums_out.shape)


def east_first_body(layers, column_ref, edge_ref, sums_ref, merid_out, energy_out):
    energy_out[...] = sums_ref[1] + east_faces(column_ref, edge_ref, layers, merid_out)


def north_last_body(
    tracers,
    row_ref,
    zonal_ref,
    last_ref,
    sums_ref,
    energy_ref,
    zonal_out,
    sums_out,
    depth_pad,
    zonal_pad,
):
    energy = north_faces(
        row_ref, zonal_ref, last_ref, energy_ref[...], zonal_out, depth_pad, zonal_pad
    )
    finish_sums(tracers, sums_ref[0], energy, sums_out)


def east_faces(column_ref, edge_ref, layers, merid_out):
    rows = STEP // 4
    lane = lax.broadcasted_iota(jnp.int32, (STEP, 128), 1)
    sublane = lax.broadcasted_iota(jnp.int32, (STEP, 128), 0)
    packed = column_ref[...]
    edge = edge_ref[...]
    own_thick, own_merid, depth, wind = (
        pltpu.roll(edge, STEP - i * rows, 0) if i else edge for i in range(4)
    )
    thick, diagonals = operator(
        lambda d: pltpu.roll(packed, -d % 128, 1),
        pltpu.roll(packed, STEP - rows, 0).astype(jnp.int32),
        pltpu.roll(packed, STEP - 2 * rows, 0),
        pltpu.roll(packed, STEP - 3 * rows, 0),
        lane,
        layers,
    )
    merid = 0.5 * (
        own_merid + apply_operator(diagonals, lambda d: pltpu.roll(wind, -d % 128, 1))
    )
    merid_out[...] = merid
    kinetic = (depth + packed) * (wind * wind) - (own_thick + thick) * (merid * merid)
    inside = (lane < layers) & (sublane < rows)
    return jnp.where(inside, 0.25 * kinetic, 0.0)


def correct_body(
    gathered_ref,
    tracer_ref,
    warmth_ref,
    zonal_ref,
    last_ref,
    merid_ref,
    edge_ref,
    tracers_out,
    warmth_out,
    zonal_out,
    merid_out,
    new_s,
    heat_s,
    merid_s,
    columns_s,
    sem,
):
    tracers = tracer_ref.shape[0]
    last = zonal_ref.shape[0] - 1
    totals = jnp.sum(gathered_ref[...], axis=0, keepdims=True)
    spread = [
        jnp.broadcast_to(totals[:, i : i + 1], (1, 128)) for i in range(tracers + 2)
    ]
    scale = 1.0 / spread[tracers + 1]
    columns_s[...] = jnp.zeros_like(columns_s)
    copies = []
    for r in range(last + 1):
        source = last_ref if r == last else zonal_ref.at[r]
        copies.append(pltpu.make_async_copy(source, zonal_out.at[r], sem.at[tracers + 1 + r]))
        copies[-1].start()
    for t in range(tracers):
        new_s[t] = tracer_ref[t] + spread[t] * scale
        copies.append(pltpu.make_async_copy(new_s.at[t], tracers_out.at[t], sem.at[t]))
        copies[-1].start()
    columns_s[pl.ds(0, STEP), :] = edge_ref[...]
    across = columns_s[...].T[0 : merid_ref.shape[1]]
    at_edge = lax.broadcasted_iota(jnp.int32, across.shape, 1) == 127
    for r in range(last + 1):
        merid_s[r] = jnp.where(at_edge, pltpu.roll(across, 127 - r, 1), merid_ref[r])
    copies.append(pltpu.make_async_copy(merid_s, merid_out, sem.at[tracers + 2 + last]))
    copies[-1].start()
    heat_s[...] = warmth_ref[...] + spread[tracers] * (scale * (1.0 / HEAT))
    copies.append(pltpu.make_async_copy(heat_s, warmth_out, sem.at[tracers]))
    copies[-1].start()
    for copy in copies:
        copy.wait()


def ring_shift(value, axis, steps):
    count = lax.axis_size(axis)
    return lax.ppermute(value, axis, [(i, (i + steps) % count) for i in range(count)])


def kernel(body, flops, moved, scratch, near, outs, operands):
    operands = [
        pltpu.with_memory_space_constraint(x, pltpu.VMEM if i in near else pltpu.HBM)
        for i, x in enumerate(operands)
    ]
    vmem = pl.BlockSpec(memory_space=pltpu.VMEM)
    hbm = pl.BlockSpec(memory_space=pl.ANY)
    return pl.pallas_call(
        body,
        out_shape=tuple(
            pltpu.VMEM(shape, jnp.float32)
            if place == "vmem"
            else jax.ShapeDtypeStruct(shape, jnp.float32)
            for shape, place in outs
        ),
        in_specs=[vmem] * len(operands),
        out_specs=tuple(hbm if place == "any" else vmem for _, place in outs),
        scratch_shapes=scratch,
        cost_estimate=pl.CostEstimate(flops=flops, bytes_accessed=moved, transcendentals=0),
        compiler_params=pltpu.CompilerParams(vmem_limit_bytes=24 * 2**20),
    )(*operands)


def local(species, zonal, merid, warmth, depth, level, start, end):
    tracers = species.shape[0]
    plane = rows, layers, columns = depth.shape
    devices = lax.axis_size(("gx", "gy"))
    tall = layers + 2 * PAD
    tile = (STEP, 128)
    real = functools.partial(pltpu.VMEM, dtype=jnp.float32)
    row_halo, column_halo = kernel(
        pack_body,
        100_000,
        600_000,
        [real((128, 128))],
        (),
        [((4, layers, columns), "vmem"), (tile, "vmem")],
        (depth, level, start, end),
    )
    column_halo = ring_shift(column_halo, "gx", -1)
    row_halo = ring_shift(row_halo, "gy", -1)
    tracer_new, warmth_new, zonal_part, merid_part, last, edge, parts = kernel(
        own_body,
        20_000_000,
        2_000_000,
        [
            real((rows, tall, columns)),
            real((rows, tall, columns)),
            real((rows, tall, columns)),
            real((rows, tall, columns)),
            real((tracers + 1, rows, tall, columns)),
            real(plane),
            real(plane),
            real((128, 128)),
        ],
        (),
        [
            ((tracers, *plane), "vmem"),
            (plane, "vmem"),
            (plane, "vmem"),
            (plane, "vmem"),
            ((3, layers, columns), "vmem"),
            (tile, "vmem"),
            ((2, *tile), "vmem"),
        ],
        (species, zonal, merid, warmth, depth, level, start, end),
    )
    merid_last, energy = kernel(
        functools.partial(east_first_body, layers),
        200_000,
        200_000,
        [],
        range(3),
        [(tile, "vmem"), (tile, "vmem")],
        (column_halo, edge, parts),
    )
    zonal_last, sums = kernel(
        functools.partial(north_last_body, tracers),
        2_000_000,
        500_000,
        [real((tall, columns)), real((tall, columns))],
        range(5),
        [((layers, columns), "vmem"), ((devices, 128), "vmem")],
        (row_halo, zonal_part, last, parts, energy),
    )
    gathered = lax.all_to_all(sums.reshape(devices, 1, 128), ("gx", "gy"), 0, 0, tiled=True)
    tracers_out, warmth_out, zonal_new, merid_new = kernel(
        correct_body,
        1_000_000,
        2_000_000,
        [
            real((tracers, *plane)),
            real(plane),
            real(plane),
            real((128, 128)),
            pltpu.SemaphoreType.DMA((tracers + 2 + rows,)),
        ],
        range(7),
        [((tracers, *plane), "any"), (plane, "any"), (plane, "any"), (plane, "any")],
        (
            gathered.reshape(devices, 128),
            tracer_new,
            warmth_new,
            zonal_part,
            zonal_last,
            merid_part,
            merid_last,
        ),
    )
    return tracers_out, zonal_new, merid_new, warmth_out


def solution(mesh):
    plane = P("gy", None, "gx")
    stack = P(None, "gy", None, "gx")
    return jax.shard_map(
        local,
        mesh=mesh,
        in_specs=(stack,) + (plane,) * 7,
        out_specs=(stack, plane, plane, plane),
        check_vma=False,
    )
```

```python
import functools

import jax
import jax.numpy as jnp
from jax import lax
from jax.experimental import pallas as pl
from jax.experimental.pallas import tpu as pltpu
from jax.sharding import Mesh
from jax.sharding import PartitionSpec as P


SPLIT = (4, 2, 2, 4, 2, 2)
NAMES = ("y", "x_hi", "z_hi", "z_lo", "x_lo", "core")
GX = NAMES[:2]
GY = NAMES[2:]
CUBE = ("y", "x_hi", "z_lo", "x_lo")

HEAT = 3.5
PAD = 8
STEP = 8
DIAGONALS = tuple(range(-4, 6))
C7 = 7.0 / 12.0
C1 = 1.0 / 12.0


def block_of(k, first=0):
    start = k * STEP + first
    return pl.ds(start if isinstance(k, int) else pl.multiple_of(start, STEP), STEP)


def padded_block(k):
    return block_of(k, PAD)


def shifted(ref, k, *lead):
    return lambda d: ref[(*lead, pl.ds(k * STEP + (PAD + d), STEP), slice(None))]


def layers_of(k):
    return lax.broadcasted_iota(jnp.int32, (STEP, 128), 0) + k * STEP


def clear_pads(ref, layers):
    lead = ref.shape[:-2]
    zero = jnp.zeros(lead + (PAD, ref.shape[-1]), ref.dtype)
    every = (slice(None),) * len(lead)
    ref[(*every, pl.ds(0, PAD), slice(None))] = zero
    ref[(*every, pl.ds(PAD + layers, PAD), slice(None))] = zero


def pick(masks, values):
    chosen = values[-1]
    for mask, value in zip(masks[-2::-1], values[-2::-1]):
        chosen = jnp.where(mask, value, chosen)
    return chosen


def operator(depth, level, start, end, target, layers):
    offset = level - target
    masks = [offset == o for o in (-2, -1, 0, 1, 2)]
    depths = [depth(d) for d in range(-2, 4)]
    weight_first = (1.0 - start) * pick(masks, depths[0:5])
    weight_second = end * pick(masks, depths[1:6])
    thick = weight_first + weight_second
    inverse = 1.0 / thick
    first = weight_first * inverse
    second = weight_second * inverse
    linear_first = 0.5 * (start + 1.0)
    square_first = linear_first - (start * start + start + 1.0) * (1.0 / 3.0)
    linear_second = 0.5 * end
    square_second = linear_second - end * end * (1.0 / 3.0)
    triple_first = 3.0 * square_first
    triple_second = 3.0 * square_second
    edge0 = first * (1.0 - linear_first - triple_first)
    edge1 = first * (linear_first - triple_first) + second * (
        1.0 - linear_second - triple_second
    )
    edge2 = second * (linear_second - triple_second)
    mean0 = first * (2.0 * triple_first)
    mean1 = second * (2.0 * triple_second)
    top, under_top = level == 0, level == 1
    bottom, over_bottom = level == layers - 2, level == layers - 3
    e0 = (
        jnp.where(top | under_top, 0.0, -C1),
        jnp.where(top, 0.0, jnp.where(under_top, 0.5, C7)),
        jnp.where(top, 1.5, jnp.where(under_top, 0.5, C7)),
        jnp.where(top, -0.5, jnp.where(under_top, 0.0, -C1)),
    )
    outer = jnp.where(top | bottom, 0.0, -C1)
    inner = jnp.where(top | bottom, 0.5, C7)
    e2 = (
        jnp.where(bottom, -0.5, jnp.where(over_bottom, 0.0, -C1)),
        jnp.where(bottom, 1.5, jnp.where(over_bottom, 0.5, C7)),
        jnp.where(bottom, 0.0, jnp.where(over_bottom, 0.5, C7)),
        jnp.where(bottom | over_bottom, 0.0, -C1),
    )
    taps = {
        -2: e0[0] * edge0,
        -1: e0[1] * edge0 + outer * edge1,
        0: e0[2] * edge0 + inner * edge1 + e2[0] * edge2 + mean0,
        1: e0[3] * edge0 + inner * edge1 + e2[1] * edge2 + mean1,
        2: outer * edge1 + e2[2] * edge2,
        3: e2[3] * edge2,
    }
    diagonals = []
    for d in DIAGONALS:
        value = jnp.zeros_like(thick)
        for mask, o in zip(masks, (-2, -1, 0, 1, 2)):
            if d - o in taps:
                value = jnp.where(mask, taps[d - o], value)
        diagonals.append(value)
    return thick, diagonals


def apply_operator(diagonals, values):
    total = None
    for d, weight in zip(DIAGONALS, diagonals):
        term = weight * values(d)
        total = term if total is None else total + term
    return total


def pack_body(depth_ref, level_ref, start_ref, end_ref, row_ref, send_ref, columns_s):
    rows, layers, columns = depth_ref.shape
    lane = lax.broadcasted_iota(jnp.int32, (layers, columns), 1)
    packed = jnp.zeros((layers, columns), jnp.float32)
    for i, ref in enumerate((depth_ref, level_ref, start_ref, end_ref)):
        for r in range(rows):
            value = ref[r].astype(jnp.float32)
            if r == 0:
                row_ref[i] = value
            place = i * rows + r
            if place:
                value = pltpu.roll(value, place, 1)
            packed = jnp.where(lane == place, value, packed)
    columns_s[pl.ds(0, layers), :] = packed
    columns_s[pl.ds(layers, 128 - layers), :] = jnp.zeros((128 - layers, 128), jnp.float32)
    send_ref[...] = columns_s[...].T[0:STEP]


def own_body(
    species_ref,
    zonal_ref,
    merid_ref,
    warmth_ref,
    depth_ref,
    level_ref,
    start_ref,
    end_ref,
    tracers_out,
    warmth_out,
    zonal_out,
    merid_out,
    last_out,
    edge_out,
    sums_out,
    depth_pad,
    zonal_pad,
    merid_pad,
    west_pad,
    field_pad,
    thick_s,
    across_s,
    columns_s,
):
    tracers = species_ref.shape[0]
    rows, layers, _ = depth_ref.shape
    blocks = layers // STEP
    for ref in (depth_pad, zonal_pad, merid_pad, west_pad, field_pad):
        clear_pads(ref, layers)

    def spread(k, carry):
        block, target = block_of(k), padded_block(k)
        for r in range(rows):
            depth_pad[r, target, :] = depth_ref[r, block, :]
            zonal_pad[r, target, :] = zonal_ref[r, block, :]
            merid_pad[r, target, :] = merid_ref[r, block, :]
            field_pad[tracers, r, target, :] = warmth_ref[r, block, :]
            for t in range(tracers):
                field_pad[t, r, target, :] = species_ref[t, r, block, :].astype(jnp.float32)
        return carry

    lax.fori_loop(0, blocks, spread, 0)
    for r in range(rows):
        west_pad[r, pl.ds(PAD, layers), :] = pltpu.roll(merid_ref[r], 1, 1)

    def own(k, carry):
        block, target = block_of(k), padded_block(k)
        lost, energy, total = list(carry[:-2]), carry[-2], carry[-1]
        thick_before = zonal_before = None
        for r in range(rows):
            thick, diagonals = operator(
                shifted(depth_pad, k, r),
                level_ref[r, block, :],
                start_ref[r, block, :].astype(jnp.float32),
                end_ref[r, block, :].astype(jnp.float32),
                layers_of(k),
                layers,
            )
            depth = depth_ref[r, block, :]
            thick_s[r, block, :] = thick
            total = total + thick
            merid_out[r, block, :] = apply_operator(diagonals, shifted(merid_pad, k, r))
            across_s[r, block, :] = apply_operator(diagonals, shifted(west_pad, k, r))
            for t in range(tracers):
                new = apply_operator(diagonals, shifted(field_pad, k, t, r))
                tracers_out[t, r, block, :] = new
                lost[t] = lost[t] + (depth * field_pad[t, r, target, :] - thick * new)
            new = apply_operator(diagonals, shifted(field_pad, k, tracers, r))
            warmth_out[r, block, :] = new
            energy = energy + HEAT * (depth * field_pad[tracers, r, target, :] - thick * new)
            zonal = apply_operator(diagonals, shifted(zonal_pad, k, r))
            if r:
                crossed = 0.5 * (
                    zonal_before + apply_operator(diagonals, shifted(zonal_pad, k, r - 1))
                )
                zonal_out[r - 1, block, :] = crossed
                wind = zonal_ref[r - 1, block, :]
                energy = energy + 0.25 * (
                    (depth_ref[r - 1, block, :] + depth) * (wind * wind)
                    - (thick_before + thick) * (crossed * crossed)
                )
            if r + 1 == rows:
                zonal_out[r, block, :] = zonal
                last_out[0, block, :] = zonal_ref[r, block, :]
                last_out[1, block, :] = depth
                last_out[2, block, :] = thick
            thick_before, zonal_before = thick, zonal
        return (*lost, energy, total)

    zero = jnp.zeros((STEP, 128), jnp.float32)
    parts = lax.fori_loop(0, blocks, own, (zero,) * (tracers + 2))

    lane = lax.broadcasted_iota(jnp.int32, (layers, 128), 1)
    columns = jnp.zeros((layers, 128), jnp.float32)
    shared = jnp.zeros((STEP, 128), jnp.float32)
    for r in range(rows):
        for i, ref in enumerate((thick_s, merid_out, depth_ref, merid_ref)):
            place = i * rows + r
            columns = jnp.where(lane == place, pltpu.roll(ref[r], place + 1, 1), columns)
        depth, thick, wind = depth_ref[r], thick_s[r], merid_ref[r]
        merid = 0.5 * (merid_out[r] + pltpu.roll(across_s[r], 127, 1))
        merid_out[r] = merid
        kinetic = (depth + pltpu.roll(depth, 127, 1)) * (wind * wind) - (
            thick + pltpu.roll(thick, 127, 1)
        ) * (merid * merid)
        shared = shared + jnp.sum(kinetic.reshape(blocks, STEP, 128), axis=0)
    columns_s[pl.ds(0, layers), :] = columns
    columns_s[pl.ds(layers, 128 - layers), :] = jnp.zeros((128 - layers, 128), jnp.float32)
    edge_out[...] = columns_s[...].T[0:STEP]

    lane = lax.broadcasted_iota(jnp.int32, (STEP, 128), 1)
    row = jnp.zeros((STEP, 128), jnp.float32)
    for i, part in enumerate(parts):
        if i != tracers:
            row = jnp.where(lane == i, jnp.sum(part, axis=1, keepdims=True), row)
    sums_out[0] = row
    sums_out[1] = parts[tracers] + jnp.where(lane == 127, 0.0, 0.25 * shared)


def north_faces(row_ref, zonal_ref, last_ref, energy, zonal_out, depth_pad, zonal_pad):
    layers = row_ref.shape[1]
    rows = zonal_ref.shape[0]
    clear_pads(depth_pad, layers)
    clear_pads(zonal_pad, layers)
    depth_pad[pl.ds(PAD, layers), :] = row_ref[0]
    zonal_pad[pl.ds(PAD, layers), :] = last_ref[0]
    for k in range(layers // STEP):
        block = block_of(k)
        thick, diagonals = operator(
            shifted(depth_pad, k),
            row_ref[1, block, :].astype(jnp.int32),
            row_ref[2, block, :],
            row_ref[3, block, :],
            layers_of(k),
            layers,
        )
        zonal = 0.5 * (
            zonal_ref[rows - 1, block, :] + apply_operator(diagonals, shifted(zonal_pad, k))
        )
        zonal_out[block, :] = zonal
        wind = last_ref[0, block, :]
        energy = energy + 0.25 * (
            (last_ref[1, block, :] + row_ref[0, block, :]) * (wind * wind)
            - (last_ref[2, block, :] + thick) * (zonal * zonal)
        )
    return energy


def finish_sums(tracers, sums, energy, sums_out):
    lane = lax.broadcasted_iota(jnp.int32, (STEP, 128), 1)
    energy = jnp.sum(energy, axis=1, keepdims=True)
    sums_out[...] = jnp.sum(jnp.where(lane == tracers, energy, sums), axis=0, keepdims=True)


def east_first_body(layers, column_ref, edge_ref, sums_ref, merid_out, energy_out):
    energy_out[...] = sums_ref[1] + east_faces(column_ref, edge_ref, layers, merid_out)


def north_last_body(
    tracers,
    row_ref,
    zonal_ref,
    last_ref,
    sums_ref,
    energy_ref,
    zonal_out,
    sums_out,
    depth_pad,
    zonal_pad,
):
    energy = north_faces(
        row_ref, zonal_ref, last_ref, energy_ref[...], zonal_out, depth_pad, zonal_pad
    )
    finish_sums(tracers, sums_ref[0], energy, sums_out)


def east_faces(column_ref, edge_ref, layers, merid_out):
    rows = STEP // 4
    lane = lax.broadcasted_iota(jnp.int32, (STEP, 128), 1)
    sublane = lax.broadcasted_iota(jnp.int32, (STEP, 128), 0)
    packed = column_ref[...]
    edge = edge_ref[...]
    own_thick, own_merid, depth, wind = (
        pltpu.roll(edge, STEP - i * rows, 0) if i else edge for i in range(4)
    )
    thick, diagonals = operator(
        lambda d: pltpu.roll(packed, -d % 128, 1),
        pltpu.roll(packed, STEP - rows, 0).astype(jnp.int32),
        pltpu.roll(packed, STEP - 2 * rows, 0),
        pltpu.roll(packed, STEP - 3 * rows, 0),
        lane,
        layers,
    )
    merid = 0.5 * (
        own_merid + apply_operator(diagonals, lambda d: pltpu.roll(wind, -d % 128, 1))
    )
    merid_out[...] = merid
    kinetic = (depth + packed) * (wind * wind) - (own_thick + thick) * (merid * merid)
    inside = (lane < layers) & (sublane < rows)
    return jnp.where(inside, 0.25 * kinetic, 0.0)


def correct_body(
    gathered_ref,
    tracer_ref,
    warmth_ref,
    zonal_ref,
    last_ref,
    merid_ref,
    edge_ref,
    tracers_out,
    warmth_out,
    zonal_out,
    merid_out,
    new_s,
    heat_s,
    merid_s,
    columns_s,
    sem,
):
    tracers = tracer_ref.shape[0]
    last = zonal_ref.shape[0] - 1
    totals = jnp.sum(gathered_ref[...], axis=0, keepdims=True)
    spread = [
        jnp.broadcast_to(totals[:, i : i + 1], (1, 128)) for i in range(tracers + 2)
    ]
    scale = 1.0 / spread[tracers + 1]
    columns_s[...] = jnp.zeros_like(columns_s)
    copies = []
    for r in range(last + 1):
        source = last_ref if r == last else zonal_ref.at[r]
        copies.append(pltpu.make_async_copy(source, zonal_out.at[r], sem.at[tracers + 1 + r]))
        copies[-1].start()
    for t in range(tracers):
        new_s[t] = tracer_ref[t] + spread[t] * scale
        copies.append(pltpu.make_async_copy(new_s.at[t], tracers_out.at[t], sem.at[t]))
        copies[-1].start()
    columns_s[pl.ds(0, STEP), :] = edge_ref[...]
    across = columns_s[...].T[0 : merid_ref.shape[1]]
    at_edge = lax.broadcasted_iota(jnp.int32, across.shape, 1) == 127
    for r in range(last + 1):
        merid_s[r] = jnp.where(at_edge, pltpu.roll(across, 127 - r, 1), merid_ref[r])
    copies.append(pltpu.make_async_copy(merid_s, merid_out, sem.at[tracers + 2 + last]))
    copies[-1].start()
    heat_s[...] = warmth_ref[...] + spread[tracers] * (scale * (1.0 / HEAT))
    copies.append(pltpu.make_async_copy(heat_s, warmth_out, sem.at[tracers]))
    copies[-1].start()
    for copy in copies:
        copy.wait()


def ring_shift(value, axis, steps):
    count = lax.axis_size(axis)
    return lax.ppermute(value, axis, [(i, (i + steps) % count) for i in range(count)])


def add_mirrored(value, axis):
    count = lax.axis_size(axis)
    return value + lax.ppermute(value, axis, [(i, count - 1 - i) for i in range(count)])


def sums_to_gather(sums):
    sums = add_mirrored(add_mirrored(sums, "core"), ("z_hi", "z_lo"))
    count = lax.axis_size(CUBE)
    rows = jnp.broadcast_to(sums[None], (count, *sums.shape))
    return lax.all_to_all(rows, CUBE, 0, 0, tiled=True).reshape(count, 128)


def kernel(body, flops, moved, scratch, near, outs, operands):
    operands = [
        pltpu.with_memory_space_constraint(x, pltpu.VMEM if i in near else pltpu.HBM)
        for i, x in enumerate(operands)
    ]
    vmem = pl.BlockSpec(memory_space=pltpu.VMEM)
    hbm = pl.BlockSpec(memory_space=pl.ANY)
    return pl.pallas_call(
        body,
        out_shape=tuple(
            pltpu.VMEM(shape, jnp.float32)
            if place == "vmem"
            else jax.ShapeDtypeStruct(shape, jnp.float32)
            for shape, place in outs
        ),
        in_specs=[vmem] * len(operands),
        out_specs=tuple(hbm if place == "any" else vmem for _, place in outs),
        scratch_shapes=scratch,
        cost_estimate=pl.CostEstimate(flops=flops, bytes_accessed=moved, transcendentals=0),
        compiler_params=pltpu.CompilerParams(vmem_limit_bytes=24 * 2**20),
    )(*operands)


def local(species, zonal, merid, warmth, depth, level, start, end):
    tracers = species.shape[0]
    plane = rows, layers, columns = depth.shape
    tall = layers + 2 * PAD
    tile = (STEP, 128)
    real = functools.partial(pltpu.VMEM, dtype=jnp.float32)
    row_halo, column_halo = kernel(
        pack_body,
        100_000,
        600_000,
        [real((128, 128))],
        (),
        [((4, layers, columns), "vmem"), (tile, "vmem")],
        (depth, level, start, end),
    )
    column_halo = ring_shift(column_halo, GX, -1)
    row_halo = ring_shift(row_halo, GY, -1)
    tracer_new, warmth_new, zonal_part, merid_part, last, edge, parts = kernel(
        own_body,
        20_000_000,
        2_000_000,
        [
            real((rows, tall, columns)),
            real((rows, tall, columns)),
            real((rows, tall, columns)),
            real((rows, tall, columns)),
            real((tracers + 1, rows, tall, columns)),
            real(plane),
            real(plane),
            real((128, 128)),
        ],
        (),
        [
            ((tracers, *plane), "vmem"),
            (plane, "vmem"),
            (plane, "vmem"),
            (plane, "vmem"),
            ((3, layers, columns), "vmem"),
            (tile, "vmem"),
            ((2, *tile), "vmem"),
        ],
        (species, zonal, merid, warmth, depth, level, start, end),
    )
    merid_last, energy = kernel(
        functools.partial(east_first_body, layers),
        200_000,
        200_000,
        [],
        range(3),
        [(tile, "vmem"), (tile, "vmem")],
        (column_halo, edge, parts),
    )
    zonal_last, sums = kernel(
        functools.partial(north_last_body, tracers),
        2_000_000,
        500_000,
        [real((tall, columns)), real((tall, columns))],
        range(5),
        [((layers, columns), "vmem"), ((1, 128), "vmem")],
        (row_halo, zonal_part, last, parts, energy),
    )
    gathered = sums_to_gather(sums)
    tracers_out, warmth_out, zonal_new, merid_new = kernel(
        correct_body,
        1_000_000,
        2_000_000,
        [
            real((tracers, *plane)),
            real(plane),
            real(plane),
            real((128, 128)),
            pltpu.SemaphoreType.DMA((tracers + 2 + rows,)),
        ],
        range(7),
        [((tracers, *plane), "any"), (plane, "any"), (plane, "any"), (plane, "any")],
        (
            gathered,
            tracer_new,
            warmth_new,
            zonal_part,
            zonal_last,
            merid_part,
            merid_last,
        ),
    )
    return tracers_out, zonal_new, merid_new, warmth_out


def solution(mesh):
    split = Mesh(mesh.devices.reshape(SPLIT), NAMES)
    plane = P(GY, None, GX)
    stack = P(None, GY, None, GX)
    return jax.shard_map(
        local,
        mesh=split,
        in_specs=(stack,) + (plane,) * 7,
        out_specs=(stack, plane, plane, plane),
        check_vma=False,
    )
```

```python
import functools

import jax
import jax.numpy as jnp
from jax import lax
from jax.experimental import pallas as pl
from jax.experimental.pallas import tpu as pltpu
from jax.sharding import Mesh
from jax.sharding import PartitionSpec as P


SPLIT = (4, 2, 2, 4, 2, 2)
NAMES = ("y", "x_hi", "z_hi", "z_lo", "x_lo", "core")
GX = NAMES[:2]
GY = NAMES[2:]
CUBE = ("y", "x_hi", "z_lo", "x_lo")

HEAT = 3.5
PAD = 8
STEP = 8
DIAGONALS = tuple(range(-4, 6))
C7 = 7.0 / 12.0
C1 = 1.0 / 12.0


def block_of(k, first=0):
    start = k * STEP + first
    return pl.ds(start if isinstance(k, int) else pl.multiple_of(start, STEP), STEP)


def padded_block(k):
    return block_of(k, PAD)


def shifted(ref, k, *lead):
    return lambda d: ref[(*lead, pl.ds(k * STEP + (PAD + d), STEP), slice(None))]


def layers_of(k):
    return lax.broadcasted_iota(jnp.int32, (STEP, 128), 0) + k * STEP


def clear_pads(ref, layers):
    lead = ref.shape[:-2]
    zero = jnp.zeros(lead + (PAD, ref.shape[-1]), ref.dtype)
    every = (slice(None),) * len(lead)
    ref[(*every, pl.ds(0, PAD), slice(None))] = zero
    ref[(*every, pl.ds(PAD + layers, PAD), slice(None))] = zero


def pick(masks, values):
    chosen = values[-1]
    for mask, value in zip(masks[-2::-1], values[-2::-1]):
        chosen = jnp.where(mask, value, chosen)
    return chosen


def operator(depth, level, start, end, target, layers):
    offset = level - target
    masks = [offset == o for o in (-2, -1, 0, 1, 2)]
    depths = [depth(d) for d in range(-2, 4)]
    weight_first = (1.0 - start) * pick(masks, depths[0:5])
    weight_second = end * pick(masks, depths[1:6])
    thick = weight_first + weight_second
    inverse = 1.0 / thick
    first = weight_first * inverse
    second = weight_second * inverse
    linear_first = 0.5 * (start + 1.0)
    square_first = linear_first - (start * start + start + 1.0) * (1.0 / 3.0)
    linear_second = 0.5 * end
    square_second = linear_second - end * end * (1.0 / 3.0)
    triple_first = 3.0 * square_first
    triple_second = 3.0 * square_second
    edge0 = first * (1.0 - linear_first - triple_first)
    edge1 = first * (linear_first - triple_first) + second * (
        1.0 - linear_second - triple_second
    )
    edge2 = second * (linear_second - triple_second)
    mean0 = first * (2.0 * triple_first)
    mean1 = second * (2.0 * triple_second)
    top, under_top = level == 0, level == 1
    bottom, over_bottom = level == layers - 2, level == layers - 3
    e0 = (
        jnp.where(top | under_top, 0.0, -C1),
        jnp.where(top, 0.0, jnp.where(under_top, 0.5, C7)),
        jnp.where(top, 1.5, jnp.where(under_top, 0.5, C7)),
        jnp.where(top, -0.5, jnp.where(under_top, 0.0, -C1)),
    )
    outer = jnp.where(top | bottom, 0.0, -C1)
    inner = jnp.where(top | bottom, 0.5, C7)
    e2 = (
        jnp.where(bottom, -0.5, jnp.where(over_bottom, 0.0, -C1)),
        jnp.where(bottom, 1.5, jnp.where(over_bottom, 0.5, C7)),
        jnp.where(bottom, 0.0, jnp.where(over_bottom, 0.5, C7)),
        jnp.where(bottom | over_bottom, 0.0, -C1),
    )
    taps = {
        -2: e0[0] * edge0,
        -1: e0[1] * edge0 + outer * edge1,
        0: e0[2] * edge0 + inner * edge1 + e2[0] * edge2 + mean0,
        1: e0[3] * edge0 + inner * edge1 + e2[1] * edge2 + mean1,
        2: outer * edge1 + e2[2] * edge2,
        3: e2[3] * edge2,
    }
    diagonals = []
    for d in DIAGONALS:
        value = jnp.zeros_like(thick)
        for mask, o in zip(masks, (-2, -1, 0, 1, 2)):
            if d - o in taps:
                value = jnp.where(mask, taps[d - o], value)
        diagonals.append(value)
    return thick, diagonals


def apply_operator(diagonals, values):
    total = None
    for d, weight in zip(DIAGONALS, diagonals):
        term = weight * values(d)
        total = term if total is None else total + term
    return total


def pack_body(depth_ref, level_ref, start_ref, end_ref, row_ref, send_ref, columns_s):
    rows, layers, columns = depth_ref.shape
    lane = lax.broadcasted_iota(jnp.int32, (layers, columns), 1)
    packed = jnp.zeros((layers, columns), jnp.float32)
    for i, ref in enumerate((depth_ref, level_ref, start_ref, end_ref)):
        for r in range(rows):
            value = ref[r].astype(jnp.float32)
            if r == 0:
                row_ref[i] = value
            place = i * rows + r
            if place:
                value = pltpu.roll(value, place, 1)
            packed = jnp.where(lane == place, value, packed)
    columns_s[pl.ds(0, layers), :] = packed
    columns_s[pl.ds(layers, 128 - layers), :] = jnp.zeros((128 - layers, 128), jnp.float32)
    send_ref[...] = columns_s[...].T[0:STEP]


def own_body(
    species_ref,
    zonal_ref,
    merid_ref,
    warmth_ref,
    depth_ref,
    level_ref,
    start_ref,
    end_ref,
    tracers_out,
    warmth_out,
    zonal_out,
    merid_out,
    last_out,
    edge_out,
    sums_out,
    depth_pad,
    zonal_pad,
    merid_pad,
    west_pad,
    field_pad,
    thick_s,
    across_s,
    columns_s,
):
    tracers = species_ref.shape[0]
    rows, layers, _ = depth_ref.shape
    blocks = layers // STEP
    for ref in (depth_pad, zonal_pad, merid_pad, west_pad, field_pad):
        clear_pads(ref, layers)

    def spread(k, carry):
        block, target = block_of(k), padded_block(k)
        for r in range(rows):
            depth_pad[r, target, :] = depth_ref[r, block, :]
            zonal_pad[r, target, :] = zonal_ref[r, block, :]
            merid_pad[r, target, :] = merid_ref[r, block, :]
            field_pad[tracers, r, target, :] = warmth_ref[r, block, :]
            for t in range(tracers):
                field_pad[t, r, target, :] = species_ref[t, r, block, :].astype(jnp.float32)
        return carry

    lax.fori_loop(0, blocks, spread, 0)
    for r in range(rows):
        west_pad[r, pl.ds(PAD, layers), :] = pltpu.roll(merid_ref[r], 1, 1)

    def own(k, carry):
        block, target = block_of(k), padded_block(k)
        lost, energy, total = list(carry[:-2]), carry[-2], carry[-1]
        thick_before = zonal_before = None
        for r in range(rows):
            thick, diagonals = operator(
                shifted(depth_pad, k, r),
                level_ref[r, block, :],
                start_ref[r, block, :].astype(jnp.float32),
                end_ref[r, block, :].astype(jnp.float32),
                layers_of(k),
                layers,
            )
            depth = depth_ref[r, block, :]
            thick_s[r, block, :] = thick
            total = total + thick
            merid_out[r, block, :] = apply_operator(diagonals, shifted(merid_pad, k, r))
            across_s[r, block, :] = apply_operator(diagonals, shifted(west_pad, k, r))
            for t in range(tracers):
                new = apply_operator(diagonals, shifted(field_pad, k, t, r))
                tracers_out[t, r, block, :] = new
                lost[t] = lost[t] + (depth * field_pad[t, r, target, :] - thick * new)
            new = apply_operator(diagonals, shifted(field_pad, k, tracers, r))
            warmth_out[r, block, :] = new
            energy = energy + HEAT * (depth * field_pad[tracers, r, target, :] - thick * new)
            zonal = apply_operator(diagonals, shifted(zonal_pad, k, r))
            if r:
                crossed = 0.5 * (
                    zonal_before + apply_operator(diagonals, shifted(zonal_pad, k, r - 1))
                )
                zonal_out[r - 1, block, :] = crossed
                wind = zonal_ref[r - 1, block, :]
                energy = energy + 0.25 * (
                    (depth_ref[r - 1, block, :] + depth) * (wind * wind)
                    - (thick_before + thick) * (crossed * crossed)
                )
            if r + 1 == rows:
                zonal_out[r, block, :] = zonal
                last_out[0, block, :] = zonal_ref[r, block, :]
                last_out[1, block, :] = depth
                last_out[2, block, :] = thick
            thick_before, zonal_before = thick, zonal
        return (*lost, energy, total)

    zero = jnp.zeros((STEP, 128), jnp.float32)
    parts = lax.fori_loop(0, blocks, own, (zero,) * (tracers + 2))

    lane = lax.broadcasted_iota(jnp.int32, (layers, 128), 1)
    columns = jnp.zeros((layers, 128), jnp.float32)
    shared = jnp.zeros((STEP, 128), jnp.float32)
    for r in range(rows):
        for i, ref in enumerate((thick_s, merid_out, depth_ref, merid_ref)):
            place = i * rows + r
            columns = jnp.where(lane == place, pltpu.roll(ref[r], place + 1, 1), columns)
        depth, thick, wind = depth_ref[r], thick_s[r], merid_ref[r]
        merid = 0.5 * (merid_out[r] + pltpu.roll(across_s[r], 127, 1))
        merid_out[r] = merid
        kinetic = (depth + pltpu.roll(depth, 127, 1)) * (wind * wind) - (
            thick + pltpu.roll(thick, 127, 1)
        ) * (merid * merid)
        shared = shared + jnp.sum(kinetic.reshape(blocks, STEP, 128), axis=0)
    columns_s[pl.ds(0, layers), :] = columns
    columns_s[pl.ds(layers, 128 - layers), :] = jnp.zeros((128 - layers, 128), jnp.float32)
    edge_out[...] = columns_s[...].T[0:STEP]

    lane = lax.broadcasted_iota(jnp.int32, (STEP, 128), 1)
    row = jnp.zeros((STEP, 128), jnp.float32)
    for i, part in enumerate(parts):
        if i != tracers:
            row = jnp.where(lane == i, jnp.sum(part, axis=1, keepdims=True), row)
    sums_out[0] = row
    sums_out[1] = parts[tracers] + jnp.where(lane == 127, 0.0, 0.25 * shared)


def north_faces(row_ref, zonal_ref, last_ref, energy, zonal_out, depth_pad, zonal_pad):
    layers = row_ref.shape[1]
    rows = zonal_ref.shape[0]
    clear_pads(depth_pad, layers)
    clear_pads(zonal_pad, layers)
    depth_pad[pl.ds(PAD, layers), :] = row_ref[0]
    zonal_pad[pl.ds(PAD, layers), :] = last_ref[0]
    for k in range(layers // STEP):
        block = block_of(k)
        thick, diagonals = operator(
            shifted(depth_pad, k),
            row_ref[1, block, :].astype(jnp.int32),
            row_ref[2, block, :],
            row_ref[3, block, :],
            layers_of(k),
            layers,
        )
        zonal = 0.5 * (
            zonal_ref[rows - 1, block, :] + apply_operator(diagonals, shifted(zonal_pad, k))
        )
        zonal_out[block, :] = zonal
        wind = last_ref[0, block, :]
        energy = energy + 0.25 * (
            (last_ref[1, block, :] + row_ref[0, block, :]) * (wind * wind)
            - (last_ref[2, block, :] + thick) * (zonal * zonal)
        )
    return energy


def finish_sums(tracers, sums, energy, sums_out):
    lane = lax.broadcasted_iota(jnp.int32, (STEP, 128), 1)
    energy = jnp.sum(energy, axis=1, keepdims=True)
    sums_out[...] = jnp.sum(jnp.where(lane == tracers, energy, sums), axis=0, keepdims=True)


def east_first_body(layers, column_ref, edge_ref, sums_ref, merid_out, energy_out):
    energy_out[...] = sums_ref[1] + east_faces(column_ref, edge_ref, layers, merid_out)


def north_last_body(
    tracers,
    row_ref,
    zonal_ref,
    last_ref,
    sums_ref,
    energy_ref,
    zonal_out,
    sums_out,
    depth_pad,
    zonal_pad,
):
    energy = north_faces(
        row_ref, zonal_ref, last_ref, energy_ref[...], zonal_out, depth_pad, zonal_pad
    )
    finish_sums(tracers, sums_ref[0], energy, sums_out)


def east_faces(column_ref, edge_ref, layers, merid_out):
    rows = STEP // 4
    lane = lax.broadcasted_iota(jnp.int32, (STEP, 128), 1)
    sublane = lax.broadcasted_iota(jnp.int32, (STEP, 128), 0)
    packed = column_ref[...]
    edge = edge_ref[...]
    own_thick, own_merid, depth, wind = (
        pltpu.roll(edge, STEP - i * rows, 0) if i else edge for i in range(4)
    )
    thick, diagonals = operator(
        lambda d: pltpu.roll(packed, -d % 128, 1),
        pltpu.roll(packed, STEP - rows, 0).astype(jnp.int32),
        pltpu.roll(packed, STEP - 2 * rows, 0),
        pltpu.roll(packed, STEP - 3 * rows, 0),
        lane,
        layers,
    )
    merid = 0.5 * (
        own_merid + apply_operator(diagonals, lambda d: pltpu.roll(wind, -d % 128, 1))
    )
    merid_out[...] = merid
    kinetic = (depth + packed) * (wind * wind) - (own_thick + thick) * (merid * merid)
    inside = (lane < layers) & (sublane < rows)
    return jnp.where(inside, 0.25 * kinetic, 0.0)


def winds_body(
    zonal_ref, last_ref, merid_ref, edge_ref, zonal_out, merid_out, merid_s, columns_s, sem
):
    rows, layers, _ = merid_ref.shape
    copies = []
    for r in range(rows):
        source = last_ref if r + 1 == rows else zonal_ref.at[r]
        copies.append(pltpu.make_async_copy(source, zonal_out.at[r], sem.at[r]))
        copies[-1].start()
    columns_s[...] = jnp.zeros_like(columns_s)
    columns_s[pl.ds(0, STEP), :] = edge_ref[...]
    across = columns_s[...].T[0:layers]
    at_edge = lax.broadcasted_iota(jnp.int32, across.shape, 1) == 127
    for r in range(rows):
        merid_s[r] = jnp.where(at_edge, pltpu.roll(across, 127 - r, 1), merid_ref[r])
    copies.append(pltpu.make_async_copy(merid_s, merid_out, sem.at[rows]))
    copies[-1].start()
    for copy in copies:
        copy.wait()


def correct_body(gathered_ref, tracer_ref, warmth_ref, tracers_out, warmth_out, new_s, heat_s, sem):
    tracers = tracer_ref.shape[0]
    totals = jnp.sum(gathered_ref[...], axis=0, keepdims=True)
    spread = [
        jnp.broadcast_to(totals[:, i : i + 1], (1, 128)) for i in range(tracers + 2)
    ]
    scale = 1.0 / spread[tracers + 1]
    copies = []
    for t in range(tracers):
        new_s[t] = tracer_ref[t] + spread[t] * scale
        copies.append(pltpu.make_async_copy(new_s.at[t], tracers_out.at[t], sem.at[t]))
        copies[-1].start()
    heat_s[...] = warmth_ref[...] + spread[tracers] * (scale * (1.0 / HEAT))
    copies.append(pltpu.make_async_copy(heat_s, warmth_out, sem.at[tracers]))
    copies[-1].start()
    for copy in copies:
        copy.wait()


def ring_shift(value, axis, steps):
    count = lax.axis_size(axis)
    return lax.ppermute(value, axis, [(i, (i + steps) % count) for i in range(count)])


def add_mirrored(value, axis):
    count = lax.axis_size(axis)
    return value + lax.ppermute(value, axis, [(i, count - 1 - i) for i in range(count)])


def sums_to_gather(sums):
    sums = add_mirrored(sums, "core")
    sums = add_mirrored(sums, ("z_hi", "z_lo"))
    count = lax.axis_size(CUBE)
    rows = jnp.broadcast_to(sums[None], (count, *sums.shape))
    return lax.all_to_all(rows, CUBE, 0, 0, tiled=True).reshape(count, 128)


def kernel(body, flops, moved, scratch, near, outs, operands):
    operands = [
        pltpu.with_memory_space_constraint(x, pltpu.VMEM if i in near else pltpu.HBM)
        for i, x in enumerate(operands)
    ]
    vmem = pl.BlockSpec(memory_space=pltpu.VMEM)
    hbm = pl.BlockSpec(memory_space=pl.ANY)
    return pl.pallas_call(
        body,
        out_shape=tuple(
            pltpu.VMEM(shape, jnp.float32)
            if place == "vmem"
            else jax.ShapeDtypeStruct(shape, jnp.float32)
            for shape, place in outs
        ),
        in_specs=[vmem] * len(operands),
        out_specs=tuple(hbm if place == "any" else vmem for _, place in outs),
        scratch_shapes=scratch,
        cost_estimate=pl.CostEstimate(flops=flops, bytes_accessed=moved, transcendentals=0),
        compiler_params=pltpu.CompilerParams(vmem_limit_bytes=24 * 2**20),
    )(*operands)


def local(species, zonal, merid, warmth, depth, level, start, end):
    tracers = species.shape[0]
    plane = rows, layers, columns = depth.shape
    tall = layers + 2 * PAD
    tile = (STEP, 128)
    real = functools.partial(pltpu.VMEM, dtype=jnp.float32)
    row_halo, column_halo = kernel(
        pack_body,
        100_000,
        600_000,
        [real((128, 128))],
        (),
        [((4, layers, columns), "vmem"), (tile, "vmem")],
        (depth, level, start, end),
    )
    column_halo = ring_shift(column_halo, GX, -1)
    row_halo = ring_shift(row_halo, GY, -1)
    tracer_new, warmth_new, zonal_part, merid_part, last, edge, parts = kernel(
        own_body,
        20_000_000,
        2_000_000,
        [
            real((rows, tall, columns)),
            real((rows, tall, columns)),
            real((rows, tall, columns)),
            real((rows, tall, columns)),
            real((tracers + 1, rows, tall, columns)),
            real(plane),
            real(plane),
            real((128, 128)),
        ],
        (),
        [
            ((tracers, *plane), "vmem"),
            (plane, "vmem"),
            (plane, "vmem"),
            (plane, "vmem"),
            ((3, layers, columns), "vmem"),
            (tile, "vmem"),
            ((2, *tile), "vmem"),
        ],
        (species, zonal, merid, warmth, depth, level, start, end),
    )
    merid_last, energy = kernel(
        functools.partial(east_first_body, layers),
        200_000,
        200_000,
        [],
        range(3),
        [(tile, "vmem"), (tile, "vmem")],
        (column_halo, edge, parts),
    )
    zonal_last, sums = kernel(
        functools.partial(north_last_body, tracers),
        2_000_000,
        500_000,
        [real((tall, columns)), real((tall, columns))],
        range(5),
        [((layers, columns), "vmem"), ((1, 128), "vmem")],
        (row_halo, zonal_part, last, parts, energy),
    )
    gathered = sums_to_gather(sums)
    zonal_new, merid_new = kernel(
        winds_body,
        200_000,
        700_000,
        [real(plane), real((128, 128)), pltpu.SemaphoreType.DMA((rows + 1,))],
        range(4),
        [(plane, "any"), (plane, "any")],
        (zonal_part, zonal_last, merid_part, merid_last),
    )
    tracers_out, warmth_out = kernel(
        correct_body,
        1_000_000,
        2_000_000,
        [real((tracers, *plane)), real(plane), pltpu.SemaphoreType.DMA((tracers + 1,))],
        range(3),
        [((tracers, *plane), "any"), (plane, "any")],
        (gathered, tracer_new, warmth_new),
    )
    return tracers_out, zonal_new, merid_new, warmth_out


def solution(mesh):
    split = Mesh(mesh.devices.reshape(SPLIT), NAMES)
    plane = P(GY, None, GX)
    stack = P(None, GY, None, GX)
    return jax.shard_map(
        local,
        mesh=split,
        in_specs=(stack,) + (plane,) * 7,
        out_specs=(stack, plane, plane, plane),
        check_vma=False,
    )
```

```python
import functools

import jax
import jax.numpy as jnp
from jax import lax
from jax.experimental import pallas as pl
from jax.experimental.pallas import tpu as pltpu
from jax.sharding import Mesh
from jax.sharding import PartitionSpec as P


SPLIT = (4, 2, 2, 4, 2, 2)
NAMES = ("y", "x_hi", "z_hi", "z_lo", "x_lo", "core")
GX = NAMES[:2]
GY = NAMES[2:]
CUBE = ("y", "x_hi", "z_lo", "x_lo")

HEAT = 3.5
PAD = 8
STEP = 8
DIAGONALS = tuple(range(-4, 6))
C7 = 7.0 / 12.0
C1 = 1.0 / 12.0


def block_of(k, first=0):
    start = k * STEP + first
    return pl.ds(start if isinstance(k, int) else pl.multiple_of(start, STEP), STEP)


def padded_block(k):
    return block_of(k, PAD)


def shifted(ref, k, *lead):
    return lambda d: ref[(*lead, pl.ds(k * STEP + (PAD + d), STEP), slice(None))]


def layers_of(k):
    return lax.broadcasted_iota(jnp.int32, (STEP, 128), 0) + k * STEP


def clear_pads(ref, layers):
    lead = ref.shape[:-2]
    zero = jnp.zeros(lead + (PAD, ref.shape[-1]), ref.dtype)
    every = (slice(None),) * len(lead)
    ref[(*every, pl.ds(0, PAD), slice(None))] = zero
    ref[(*every, pl.ds(PAD + layers, PAD), slice(None))] = zero


def pick(masks, values):
    chosen = values[-1]
    for mask, value in zip(masks[-2::-1], values[-2::-1]):
        chosen = jnp.where(mask, value, chosen)
    return chosen


def operator(depth, level, start, end, target, layers, ends=True):
    offset = level - target
    masks = [offset == o for o in (-2, -1, 0, 1, 2)]
    depths = [depth(d) for d in range(-2, 4)]
    weight_first = (1.0 - start) * pick(masks, depths[0:5])
    weight_second = end * pick(masks, depths[1:6])
    thick = weight_first + weight_second
    inverse = 1.0 / thick
    first = weight_first * inverse
    second = weight_second * inverse
    linear_first = 0.5 * (start + 1.0)
    square_first = linear_first - (start * start + start + 1.0) * (1.0 / 3.0)
    linear_second = 0.5 * end
    square_second = linear_second - end * end * (1.0 / 3.0)
    triple_first = 3.0 * square_first
    triple_second = 3.0 * square_second
    edge0 = first * (1.0 - linear_first - triple_first)
    edge1 = first * (linear_first - triple_first) + second * (
        1.0 - linear_second - triple_second
    )
    edge2 = second * (linear_second - triple_second)
    mean0 = first * (2.0 * triple_first)
    mean1 = second * (2.0 * triple_second)
    if ends:
        top, under_top = level == 0, level == 1
        bottom, over_bottom = level == layers - 2, level == layers - 3
        e0 = (
            jnp.where(top | under_top, 0.0, -C1),
            jnp.where(top, 0.0, jnp.where(under_top, 0.5, C7)),
            jnp.where(top, 1.5, jnp.where(under_top, 0.5, C7)),
            jnp.where(top, -0.5, jnp.where(under_top, 0.0, -C1)),
        )
        outer = jnp.where(top | bottom, 0.0, -C1)
        inner = jnp.where(top | bottom, 0.5, C7)
        e2 = (
            jnp.where(bottom, -0.5, jnp.where(over_bottom, 0.0, -C1)),
            jnp.where(bottom, 1.5, jnp.where(over_bottom, 0.5, C7)),
            jnp.where(bottom, 0.0, jnp.where(over_bottom, 0.5, C7)),
            jnp.where(bottom | over_bottom, 0.0, -C1),
        )
    else:
        e0 = e2 = (-C1, C7, C7, -C1)
        outer, inner = -C1, C7
    taps = {
        -2: e0[0] * edge0,
        -1: e0[1] * edge0 + outer * edge1,
        0: e0[2] * edge0 + inner * edge1 + e2[0] * edge2 + mean0,
        1: e0[3] * edge0 + inner * edge1 + e2[1] * edge2 + mean1,
        2: outer * edge1 + e2[2] * edge2,
        3: e2[3] * edge2,
    }
    diagonals = []
    for d in DIAGONALS:
        value = jnp.zeros_like(thick)
        for mask, o in zip(masks, (-2, -1, 0, 1, 2)):
            if d - o in taps:
                value = jnp.where(mask, taps[d - o], value)
        diagonals.append(value)
    return thick, diagonals


def apply_operator(diagonals, values):
    total = None
    for d, weight in zip(DIAGONALS, diagonals):
        term = weight * values(d)
        total = term if total is None else total + term
    return total


def pack_body(depth_ref, level_ref, start_ref, end_ref, row_ref, send_ref, columns_s):
    rows, layers, columns = depth_ref.shape
    lane = lax.broadcasted_iota(jnp.int32, (layers, columns), 1)
    packed = jnp.zeros((layers, columns), jnp.float32)
    for i, ref in enumerate((depth_ref, level_ref, start_ref, end_ref)):
        for r in range(rows):
            value = ref[r].astype(jnp.float32)
            if r == 0:
                row_ref[i] = value
            place = i * rows + r
            if place:
                value = pltpu.roll(value, place, 1)
            packed = jnp.where(lane == place, value, packed)
    columns_s[pl.ds(0, layers), :] = packed
    columns_s[pl.ds(layers, 128 - layers), :] = jnp.zeros((128 - layers, 128), jnp.float32)
    send_ref[...] = columns_s[...].T[0:STEP]


def own_body(
    species_ref,
    zonal_ref,
    merid_ref,
    warmth_ref,
    depth_ref,
    level_ref,
    start_ref,
    end_ref,
    tracers_out,
    warmth_out,
    zonal_out,
    merid_out,
    last_out,
    edge_out,
    sums_out,
    depth_pad,
    zonal_pad,
    merid_pad,
    west_pad,
    field_pad,
    thick_s,
    across_s,
    columns_s,
):
    tracers = species_ref.shape[0]
    rows, layers, _ = depth_ref.shape
    blocks = layers // STEP
    for ref in (depth_pad, zonal_pad, merid_pad, west_pad, field_pad):
        clear_pads(ref, layers)

    def spread(k, carry):
        block, target = block_of(k), padded_block(k)
        for r in range(rows):
            depth_pad[r, target, :] = depth_ref[r, block, :]
            zonal_pad[r, target, :] = zonal_ref[r, block, :]
            merid_pad[r, target, :] = merid_ref[r, block, :]
            field_pad[tracers, r, target, :] = warmth_ref[r, block, :]
            for t in range(tracers):
                field_pad[t, r, target, :] = species_ref[t, r, block, :].astype(jnp.float32)
        return carry

    lax.fori_loop(0, blocks, spread, 0)
    for r in range(rows):
        west_pad[r, pl.ds(PAD, layers), :] = pltpu.roll(merid_ref[r], 1, 1)

    def own(k, carry):
        block, target = block_of(k), padded_block(k)
        lost, energy, total = list(carry[:-2]), carry[-2], carry[-1]
        thick_before = zonal_before = None
        for r in range(rows):
            thick, diagonals = operator(
                shifted(depth_pad, k, r),
                level_ref[r, block, :],
                start_ref[r, block, :].astype(jnp.float32),
                end_ref[r, block, :].astype(jnp.float32),
                layers_of(k),
                layers,
            )
            depth = depth_ref[r, block, :]
            thick_s[r, block, :] = thick
            total = total + thick
            merid_out[r, block, :] = apply_operator(diagonals, shifted(merid_pad, k, r))
            across_s[r, block, :] = apply_operator(diagonals, shifted(west_pad, k, r))
            for t in range(tracers):
                new = apply_operator(diagonals, shifted(field_pad, k, t, r))
                tracers_out[t, r, block, :] = new
                lost[t] = lost[t] + (depth * field_pad[t, r, target, :] - thick * new)
            new = apply_operator(diagonals, shifted(field_pad, k, tracers, r))
            warmth_out[r, block, :] = new
            energy = energy + HEAT * (depth * field_pad[tracers, r, target, :] - thick * new)
            zonal = apply_operator(diagonals, shifted(zonal_pad, k, r))
            if r:
                crossed = 0.5 * (
                    zonal_before + apply_operator(diagonals, shifted(zonal_pad, k, r - 1))
                )
                zonal_out[r - 1, block, :] = crossed
                wind = zonal_ref[r - 1, block, :]
                energy = energy + 0.25 * (
                    (depth_ref[r - 1, block, :] + depth) * (wind * wind)
                    - (thick_before + thick) * (crossed * crossed)
                )
            if r + 1 == rows:
                zonal_out[r, block, :] = zonal
                last_out[0, block, :] = zonal_ref[r, block, :]
                last_out[1, block, :] = depth
                last_out[2, block, :] = thick
            thick_before, zonal_before = thick, zonal
        return (*lost, energy, total)

    zero = jnp.zeros((STEP, 128), jnp.float32)
    parts = lax.fori_loop(0, blocks, own, (zero,) * (tracers + 2))

    lane = lax.broadcasted_iota(jnp.int32, (layers, 128), 1)
    columns = jnp.zeros((layers, 128), jnp.float32)
    shared = jnp.zeros((STEP, 128), jnp.float32)
    for r in range(rows):
        for i, ref in enumerate((thick_s, merid_out, depth_ref, merid_ref)):
            place = i * rows + r
            columns = jnp.where(lane == place, pltpu.roll(ref[r], place + 1, 1), columns)
        depth, thick, wind = depth_ref[r], thick_s[r], merid_ref[r]
        merid = 0.5 * (merid_out[r] + pltpu.roll(across_s[r], 127, 1))
        merid_out[r] = merid
        kinetic = (depth + pltpu.roll(depth, 127, 1)) * (wind * wind) - (
            thick + pltpu.roll(thick, 127, 1)
        ) * (merid * merid)
        shared = shared + jnp.sum(kinetic.reshape(blocks, STEP, 128), axis=0)
    columns_s[pl.ds(0, layers), :] = columns
    columns_s[pl.ds(layers, 128 - layers), :] = jnp.zeros((128 - layers, 128), jnp.float32)
    edge_out[...] = columns_s[...].T[0:STEP]

    lane = lax.broadcasted_iota(jnp.int32, (STEP, 128), 1)
    row = jnp.zeros((STEP, 128), jnp.float32)
    for i, part in enumerate(parts):
        if i != tracers:
            row = jnp.where(lane == i, jnp.sum(part, axis=1, keepdims=True), row)
    sums_out[0] = row
    sums_out[1] = parts[tracers] + jnp.where(lane == 127, 0.0, 0.25 * shared)


def north_faces(row_ref, zonal_ref, last_ref, energy, zonal_out, depth_pad, zonal_pad):
    layers = row_ref.shape[1]
    rows = zonal_ref.shape[0]
    clear_pads(depth_pad, layers)
    clear_pads(zonal_pad, layers)
    depth_pad[pl.ds(PAD, layers), :] = row_ref[0]
    zonal_pad[pl.ds(PAD, layers), :] = last_ref[0]
    for k in range(layers // STEP):
        block = block_of(k)
        thick, diagonals = operator(
            shifted(depth_pad, k),
            row_ref[1, block, :].astype(jnp.int32),
            row_ref[2, block, :],
            row_ref[3, block, :],
            layers_of(k),
            layers,
            ends=k in (0, layers // STEP - 1),
        )
        zonal = 0.5 * (
            zonal_ref[rows - 1, block, :] + apply_operator(diagonals, shifted(zonal_pad, k))
        )
        zonal_out[block, :] = zonal
        wind = last_ref[0, block, :]
        energy = energy + 0.25 * (
            (last_ref[1, block, :] + row_ref[0, block, :]) * (wind * wind)
            - (last_ref[2, block, :] + thick) * (zonal * zonal)
        )
    return energy


def finish_sums(tracers, sums, energy, sums_out):
    lane = lax.broadcasted_iota(jnp.int32, (STEP, 128), 1)
    energy = jnp.sum(energy, axis=1, keepdims=True)
    sums_out[...] = jnp.sum(jnp.where(lane == tracers, energy, sums), axis=0, keepdims=True)


def east_first_body(layers, column_ref, edge_ref, sums_ref, merid_out, energy_out):
    energy_out[...] = sums_ref[1] + east_faces(column_ref, edge_ref, layers, merid_out)


def north_last_body(
    tracers,
    row_ref,
    zonal_ref,
    last_ref,
    sums_ref,
    energy_ref,
    zonal_out,
    sums_out,
    depth_pad,
    zonal_pad,
):
    energy = north_faces(
        row_ref, zonal_ref, last_ref, energy_ref[...], zonal_out, depth_pad, zonal_pad
    )
    finish_sums(tracers, sums_ref[0], energy, sums_out)


def east_faces(column_ref, edge_ref, layers, merid_out):
    rows = STEP // 4
    lane = lax.broadcasted_iota(jnp.int32, (STEP, 128), 1)
    sublane = lax.broadcasted_iota(jnp.int32, (STEP, 128), 0)
    packed = column_ref[...]
    edge = edge_ref[...]
    own_thick, own_merid, depth, wind = (
        pltpu.roll(edge, STEP - i * rows, 0) if i else edge for i in range(4)
    )
    thick, diagonals = operator(
        lambda d: pltpu.roll(packed, -d % 128, 1),
        pltpu.roll(packed, STEP - rows, 0).astype(jnp.int32),
        pltpu.roll(packed, STEP - 2 * rows, 0),
        pltpu.roll(packed, STEP - 3 * rows, 0),
        lane,
        layers,
    )
    merid = 0.5 * (
        own_merid + apply_operator(diagonals, lambda d: pltpu.roll(wind, -d % 128, 1))
    )
    merid_out[...] = merid
    kinetic = (depth + packed) * (wind * wind) - (own_thick + thick) * (merid * merid)
    inside = (lane < layers) & (sublane < rows)
    return jnp.where(inside, 0.25 * kinetic, 0.0)


def winds_body(
    zonal_ref, last_ref, merid_ref, edge_ref, zonal_out, merid_out, merid_s, columns_s, sem
):
    rows, layers, _ = merid_ref.shape
    copies = []
    for r in range(rows):
        source = last_ref if r + 1 == rows else zonal_ref.at[r]
        copies.append(pltpu.make_async_copy(source, zonal_out.at[r], sem.at[r]))
        copies[-1].start()
    columns_s[...] = jnp.zeros_like(columns_s)
    columns_s[pl.ds(0, STEP), :] = edge_ref[...]
    across = columns_s[...].T[0:layers]
    at_edge = lax.broadcasted_iota(jnp.int32, across.shape, 1) == 127
    for r in range(rows):
        merid_s[r] = jnp.where(at_edge, pltpu.roll(across, 127 - r, 1), merid_ref[r])
    copies.append(pltpu.make_async_copy(merid_s, merid_out, sem.at[rows]))
    copies[-1].start()
    for copy in copies:
        copy.wait()


def correct_body(gathered_ref, tracer_ref, warmth_ref, tracers_out, warmth_out, new_s, heat_s, sem):
    tracers = tracer_ref.shape[0]
    totals = jnp.sum(gathered_ref[...], axis=0, keepdims=True)
    spread = [
        jnp.broadcast_to(totals[:, i : i + 1], (1, 128)) for i in range(tracers + 2)
    ]
    scale = 1.0 / spread[tracers + 1]
    copies = []
    for t in range(tracers):
        new_s[t] = tracer_ref[t] + spread[t] * scale
        copies.append(pltpu.make_async_copy(new_s.at[t], tracers_out.at[t], sem.at[t]))
        copies[-1].start()
    heat_s[...] = warmth_ref[...] + spread[tracers] * (scale * (1.0 / HEAT))
    copies.append(pltpu.make_async_copy(heat_s, warmth_out, sem.at[tracers]))
    copies[-1].start()
    for copy in copies:
        copy.wait()


def ring_shift(value, axis, steps):
    count = lax.axis_size(axis)
    return lax.ppermute(value, axis, [(i, (i + steps) % count) for i in range(count)])


def add_mirrored(value, axis):
    count = lax.axis_size(axis)
    return value + lax.ppermute(value, axis, [(i, count - 1 - i) for i in range(count)])


def sums_to_gather(sums):
    sums = add_mirrored(sums, "core")
    sums = add_mirrored(sums, ("z_hi", "z_lo"))
    count = lax.axis_size(CUBE)
    rows = jnp.broadcast_to(sums[None], (count, *sums.shape))
    return lax.all_to_all(rows, CUBE, 0, 0, tiled=True).reshape(count, 128)


def kernel(body, flops, moved, scratch, near, outs, operands):
    operands = [
        pltpu.with_memory_space_constraint(x, pltpu.VMEM if i in near else pltpu.HBM)
        for i, x in enumerate(operands)
    ]
    vmem = pl.BlockSpec(memory_space=pltpu.VMEM)
    hbm = pl.BlockSpec(memory_space=pl.ANY)
    return pl.pallas_call(
        body,
        out_shape=tuple(
            pltpu.VMEM(shape, jnp.float32)
            if place == "vmem"
            else jax.ShapeDtypeStruct(shape, jnp.float32)
            for shape, place in outs
        ),
        in_specs=[vmem] * len(operands),
        out_specs=tuple(hbm if place == "any" else vmem for _, place in outs),
        scratch_shapes=scratch,
        cost_estimate=pl.CostEstimate(flops=flops, bytes_accessed=moved, transcendentals=0),
        compiler_params=pltpu.CompilerParams(vmem_limit_bytes=24 * 2**20),
    )(*operands)


def local(species, zonal, merid, warmth, depth, level, start, end):
    tracers = species.shape[0]
    plane = rows, layers, columns = depth.shape
    tall = layers + 2 * PAD
    tile = (STEP, 128)
    real = functools.partial(pltpu.VMEM, dtype=jnp.float32)
    row_halo, column_halo = kernel(
        pack_body,
        100_000,
        600_000,
        [real((128, 128))],
        (),
        [((4, layers, columns), "vmem"), (tile, "vmem")],
        (depth, level, start, end),
    )
    column_halo = ring_shift(column_halo, GX, -1)
    row_halo = ring_shift(row_halo, GY, -1)
    tracer_new, warmth_new, zonal_part, merid_part, last, edge, parts = kernel(
        own_body,
        20_000_000,
        2_000_000,
        [
            real((rows, tall, columns)),
            real((rows, tall, columns)),
            real((rows, tall, columns)),
            real((rows, tall, columns)),
            real((tracers + 1, rows, tall, columns)),
            real(plane),
            real(plane),
            real((128, 128)),
        ],
        (),
        [
            ((tracers, *plane), "vmem"),
            (plane, "vmem"),
            (plane, "vmem"),
            (plane, "vmem"),
            ((3, layers, columns), "vmem"),
            (tile, "vmem"),
            ((2, *tile), "vmem"),
        ],
        (species, zonal, merid, warmth, depth, level, start, end),
    )
    merid_last, energy = kernel(
        functools.partial(east_first_body, layers),
        200_000,
        200_000,
        [],
        range(3),
        [(tile, "vmem"), (tile, "vmem")],
        (column_halo, edge, parts),
    )
    zonal_last, sums = kernel(
        functools.partial(north_last_body, tracers),
        2_000_000,
        500_000,
        [real((tall, columns)), real((tall, columns))],
        range(5),
        [((layers, columns), "vmem"), ((1, 128), "vmem")],
        (row_halo, zonal_part, last, parts, energy),
    )
    gathered = sums_to_gather(sums)
    zonal_new, merid_new = kernel(
        winds_body,
        200_000,
        700_000,
        [real(plane), real((128, 128)), pltpu.SemaphoreType.DMA((rows + 1,))],
        range(4),
        [(plane, "any"), (plane, "any")],
        (zonal_part, zonal_last, merid_part, merid_last),
    )
    tracers_out, warmth_out = kernel(
        correct_body,
        1_000_000,
        2_000_000,
        [real((tracers, *plane)), real(plane), pltpu.SemaphoreType.DMA((tracers + 1,))],
        range(3),
        [((tracers, *plane), "any"), (plane, "any")],
        (gathered, tracer_new, warmth_new),
    )
    return tracers_out, zonal_new, merid_new, warmth_out


def solution(mesh):
    split = Mesh(mesh.devices.reshape(SPLIT), NAMES)
    plane = P(GY, None, GX)
    stack = P(None, GY, None, GX)
    return jax.shard_map(
        local,
        mesh=split,
        in_specs=(stack,) + (plane,) * 7,
        out_specs=(stack, plane, plane, plane),
        check_vma=False,
    )
```

```python
import functools

import jax
import jax.numpy as jnp
from jax import lax
from jax.experimental import pallas as pl
from jax.experimental.pallas import tpu as pltpu
from jax.sharding import Mesh
from jax.sharding import PartitionSpec as P


SPLIT = (4, 2, 2, 4, 2, 2)
NAMES = ("y", "x_hi", "z_hi", "z_lo", "x_lo", "core")
GX = NAMES[:2]
GY = NAMES[2:]
CUBE = ("y", "x_hi", "z_lo", "x_lo")

HEAT = 3.5
PAD = 8
STEP = 8
DIAGONALS = tuple(range(-4, 6))
C7 = 7.0 / 12.0
C1 = 1.0 / 12.0


def block_of(k, first=0):
    start = k * STEP + first
    return pl.ds(start if isinstance(k, int) else pl.multiple_of(start, STEP), STEP)


def padded_block(k):
    return block_of(k, PAD)


def shifted(ref, k, *lead):
    return lambda d: ref[(*lead, pl.ds(k * STEP + (PAD + d), STEP), slice(None))]


def layers_of(k):
    return lax.broadcasted_iota(jnp.int32, (STEP, 128), 0) + k * STEP


def clear_pads(ref, layers):
    lead = ref.shape[:-2]
    zero = jnp.zeros(lead + (PAD, ref.shape[-1]), ref.dtype)
    every = (slice(None),) * len(lead)
    ref[(*every, pl.ds(0, PAD), slice(None))] = zero
    ref[(*every, pl.ds(PAD + layers, PAD), slice(None))] = zero


def pick(masks, values):
    chosen = values[-1]
    for mask, value in zip(masks[-2::-1], values[-2::-1]):
        chosen = jnp.where(mask, value, chosen)
    return chosen


def operator(depth, level, start, end, target, layers, ends=True):
    offset = level - target
    masks = [offset == o for o in (-2, -1, 0, 1, 2)]
    depths = [depth(d) for d in range(-2, 4)]
    weight_first = (1.0 - start) * pick(masks, depths[0:5])
    weight_second = end * pick(masks, depths[1:6])
    thick = weight_first + weight_second
    inverse = 1.0 / thick
    first = weight_first * inverse
    second = weight_second * inverse
    linear_first = 0.5 * (start + 1.0)
    square_first = linear_first - (start * start + start + 1.0) * (1.0 / 3.0)
    linear_second = 0.5 * end
    square_second = linear_second - end * end * (1.0 / 3.0)
    triple_first = 3.0 * square_first
    triple_second = 3.0 * square_second
    edge0 = first * (1.0 - linear_first - triple_first)
    edge1 = first * (linear_first - triple_first) + second * (
        1.0 - linear_second - triple_second
    )
    edge2 = second * (linear_second - triple_second)
    mean0 = first * (2.0 * triple_first)
    mean1 = second * (2.0 * triple_second)
    if ends:
        top, under_top = level == 0, level == 1
        bottom, over_bottom = level == layers - 2, level == layers - 3
        e0 = (
            jnp.where(top | under_top, 0.0, -C1),
            jnp.where(top, 0.0, jnp.where(under_top, 0.5, C7)),
            jnp.where(top, 1.5, jnp.where(under_top, 0.5, C7)),
            jnp.where(top, -0.5, jnp.where(under_top, 0.0, -C1)),
        )
        outer = jnp.where(top | bottom, 0.0, -C1)
        inner = jnp.where(top | bottom, 0.5, C7)
        e2 = (
            jnp.where(bottom, -0.5, jnp.where(over_bottom, 0.0, -C1)),
            jnp.where(bottom, 1.5, jnp.where(over_bottom, 0.5, C7)),
            jnp.where(bottom, 0.0, jnp.where(over_bottom, 0.5, C7)),
            jnp.where(bottom | over_bottom, 0.0, -C1),
        )
    else:
        e0 = e2 = (-C1, C7, C7, -C1)
        outer, inner = -C1, C7
    taps = {
        -2: e0[0] * edge0,
        -1: e0[1] * edge0 + outer * edge1,
        0: e0[2] * edge0 + inner * edge1 + e2[0] * edge2 + mean0,
        1: e0[3] * edge0 + inner * edge1 + e2[1] * edge2 + mean1,
        2: outer * edge1 + e2[2] * edge2,
        3: e2[3] * edge2,
    }
    diagonals = []
    for d in DIAGONALS:
        value = jnp.zeros_like(thick)
        for mask, o in zip(masks, (-2, -1, 0, 1, 2)):
            if d - o in taps:
                value = jnp.where(mask, taps[d - o], value)
        diagonals.append(value)
    return thick, diagonals


def apply_operator(diagonals, values):
    total = None
    for d, weight in zip(DIAGONALS, diagonals):
        term = weight * values(d)
        total = term if total is None else total + term
    return total


def pack_body(depth_ref, level_ref, start_ref, end_ref, row_ref, send_ref, columns_s):
    rows, layers, columns = depth_ref.shape
    lane = lax.broadcasted_iota(jnp.int32, (layers, columns), 1)
    packed = jnp.zeros((layers, columns), jnp.float32)
    for i, ref in enumerate((depth_ref, level_ref, start_ref, end_ref)):
        for r in range(rows):
            value = ref[r].astype(jnp.float32)
            if r == 0:
                row_ref[i] = value
            place = i * rows + r
            if place:
                value = pltpu.roll(value, place, 1)
            packed = jnp.where(lane == place, value, packed)
    columns_s[pl.ds(0, layers), :] = packed
    columns_s[pl.ds(layers, 128 - layers), :] = jnp.zeros((128 - layers, 128), jnp.float32)
    send_ref[...] = columns_s[...].T[0:STEP]


def own_body(
    species_ref,
    zonal_ref,
    merid_ref,
    warmth_ref,
    depth_ref,
    level_ref,
    start_ref,
    end_ref,
    tracers_out,
    warmth_out,
    zonal_out,
    merid_out,
    last_out,
    edge_out,
    sums_out,
    depth_pad,
    zonal_pad,
    merid_pad,
    west_pad,
    field_pad,
    thick_s,
    across_s,
    columns_s,
):
    tracers = species_ref.shape[0]
    rows, layers, _ = depth_ref.shape
    blocks = layers // STEP
    for ref in (depth_pad, zonal_pad, merid_pad, west_pad, field_pad):
        clear_pads(ref, layers)

    def spread(k, carry):
        block, target = block_of(k), padded_block(k)
        for r in range(rows):
            depth_pad[r, target, :] = depth_ref[r, block, :]
            zonal_pad[r, target, :] = zonal_ref[r, block, :]
            merid_pad[r, target, :] = merid_ref[r, block, :]
            field_pad[tracers, r, target, :] = warmth_ref[r, block, :]
            for t in range(tracers):
                field_pad[t, r, target, :] = species_ref[t, r, block, :].astype(jnp.float32)
        return carry

    lax.fori_loop(0, blocks, spread, 0)
    for r in range(rows):
        west_pad[r, pl.ds(PAD, layers), :] = pltpu.roll(merid_ref[r], 1, 1)

    def own(k, carry):
        block, target = block_of(k), padded_block(k)
        lost, energy, total = list(carry[:-2]), carry[-2], carry[-1]
        thick_before = zonal_before = None
        for r in range(rows):
            thick, diagonals = operator(
                shifted(depth_pad, k, r),
                level_ref[r, block, :],
                start_ref[r, block, :].astype(jnp.float32),
                end_ref[r, block, :].astype(jnp.float32),
                layers_of(k),
                layers,
            )
            depth = depth_ref[r, block, :]
            thick_s[r, block, :] = thick
            total = total + thick
            merid_out[r, block, :] = apply_operator(diagonals, shifted(merid_pad, k, r))
            across_s[r, block, :] = apply_operator(diagonals, shifted(west_pad, k, r))
            for t in range(tracers):
                new = apply_operator(diagonals, shifted(field_pad, k, t, r))
                tracers_out[t, r, block, :] = new
                lost[t] = lost[t] + (depth * field_pad[t, r, target, :] - thick * new)
            new = apply_operator(diagonals, shifted(field_pad, k, tracers, r))
            warmth_out[r, block, :] = new
            energy = energy + HEAT * (depth * field_pad[tracers, r, target, :] - thick * new)
            zonal = apply_operator(diagonals, shifted(zonal_pad, k, r))
            if r:
                crossed = 0.5 * (
                    zonal_before + apply_operator(diagonals, shifted(zonal_pad, k, r - 1))
                )
                zonal_out[r - 1, block, :] = crossed
                wind = zonal_ref[r - 1, block, :]
                energy = energy + 0.25 * (
                    (depth_ref[r - 1, block, :] + depth) * (wind * wind)
                    - (thick_before + thick) * (crossed * crossed)
                )
            if r + 1 == rows:
                zonal_out[r, block, :] = zonal
                last_out[0, block, :] = zonal_ref[r, block, :]
                last_out[1, block, :] = depth
                last_out[2, block, :] = thick
            thick_before, zonal_before = thick, zonal
        return (*lost, energy, total)

    zero = jnp.zeros((STEP, 128), jnp.float32)
    parts = lax.fori_loop(0, blocks, own, (zero,) * (tracers + 2))

    lane = lax.broadcasted_iota(jnp.int32, (layers, 128), 1)
    columns = jnp.zeros((layers, 128), jnp.float32)
    shared = jnp.zeros((STEP, 128), jnp.float32)
    for r in range(rows):
        for i, ref in enumerate((thick_s, merid_out, depth_ref, merid_ref)):
            place = i * rows + r
            columns = jnp.where(lane == place, pltpu.roll(ref[r], place + 1, 1), columns)
        depth, thick, wind = depth_ref[r], thick_s[r], merid_ref[r]
        merid = 0.5 * (merid_out[r] + pltpu.roll(across_s[r], 127, 1))
        merid_out[r] = merid
        kinetic = (depth + pltpu.roll(depth, 127, 1)) * (wind * wind) - (
            thick + pltpu.roll(thick, 127, 1)
        ) * (merid * merid)
        shared = shared + jnp.sum(kinetic.reshape(blocks, STEP, 128), axis=0)
    columns_s[pl.ds(0, layers), :] = columns
    columns_s[pl.ds(layers, 128 - layers), :] = jnp.zeros((128 - layers, 128), jnp.float32)
    edge_out[...] = columns_s[...].T[0:STEP]

    lane = lax.broadcasted_iota(jnp.int32, (STEP, 128), 1)
    row = jnp.zeros((STEP, 128), jnp.float32)
    for i, part in enumerate(parts):
        if i != tracers:
            row = jnp.where(lane == i, jnp.sum(part, axis=1, keepdims=True), row)
    sums_out[0] = row
    sums_out[1] = parts[tracers] + jnp.where(lane == 127, 0.0, 0.25 * shared)


def north_faces(row_ref, zonal_ref, last_ref, energy, zonal_out, depth_pad, zonal_pad):
    layers = row_ref.shape[1]
    rows = zonal_ref.shape[0]
    clear_pads(depth_pad, layers)
    clear_pads(zonal_pad, layers)
    depth_pad[pl.ds(PAD, layers), :] = row_ref[0]
    zonal_pad[pl.ds(PAD, layers), :] = last_ref[0]
    for k in range(layers // STEP):
        block = block_of(k)
        thick, diagonals = operator(
            shifted(depth_pad, k),
            row_ref[1, block, :].astype(jnp.int32),
            row_ref[2, block, :],
            row_ref[3, block, :],
            layers_of(k),
            layers,
            ends=k in (0, layers // STEP - 1),
        )
        zonal = 0.5 * (
            zonal_ref[rows - 1, block, :] + apply_operator(diagonals, shifted(zonal_pad, k))
        )
        zonal_out[block, :] = zonal
        wind = last_ref[0, block, :]
        energy = energy + 0.25 * (
            (last_ref[1, block, :] + row_ref[0, block, :]) * (wind * wind)
            - (last_ref[2, block, :] + thick) * (zonal * zonal)
        )
    return energy


def finish_sums(tracers, sums, energy, sums_out):
    lane = lax.broadcasted_iota(jnp.int32, (STEP, 128), 1)
    energy = jnp.sum(energy, axis=1, keepdims=True)
    sums_out[...] = jnp.sum(jnp.where(lane == tracers, energy, sums), axis=0, keepdims=True)


def east_first_body(layers, column_ref, edge_ref, sums_ref, merid_out, energy_out):
    energy_out[...] = sums_ref[1] + east_faces(column_ref, edge_ref, layers, merid_out)


def north_last_body(
    tracers,
    row_ref,
    zonal_ref,
    last_ref,
    sums_ref,
    energy_ref,
    zonal_out,
    sums_out,
    depth_pad,
    zonal_pad,
):
    energy = north_faces(
        row_ref, zonal_ref, last_ref, energy_ref[...], zonal_out, depth_pad, zonal_pad
    )
    finish_sums(tracers, sums_ref[0], energy, sums_out)


def east_faces(column_ref, edge_ref, layers, merid_out):
    rows = STEP // 4
    lane = lax.broadcasted_iota(jnp.int32, (STEP, 128), 1)
    sublane = lax.broadcasted_iota(jnp.int32, (STEP, 128), 0)
    packed = column_ref[...]
    edge = edge_ref[...]
    own_thick, own_merid, depth, wind = (
        pltpu.roll(edge, STEP - i * rows, 0) if i else edge for i in range(4)
    )
    thick, diagonals = operator(
        lambda d: pltpu.roll(packed, -d % 128, 1),
        pltpu.roll(packed, STEP - rows, 0).astype(jnp.int32),
        pltpu.roll(packed, STEP - 2 * rows, 0),
        pltpu.roll(packed, STEP - 3 * rows, 0),
        lane,
        layers,
    )
    merid = 0.5 * (
        own_merid + apply_operator(diagonals, lambda d: pltpu.roll(wind, -d % 128, 1))
    )
    merid_out[...] = merid
    kinetic = (depth + packed) * (wind * wind) - (own_thick + thick) * (merid * merid)
    inside = (lane < layers) & (sublane < rows)
    return jnp.where(inside, 0.25 * kinetic, 0.0)


def winds_body(
    zonal_ref, last_ref, merid_ref, edge_ref, zonal_out, merid_out, merid_s, columns_s, sem
):
    rows, layers, _ = merid_ref.shape
    copies = []
    for r in range(rows):
        source = last_ref if r + 1 == rows else zonal_ref.at[r]
        copies.append(pltpu.make_async_copy(source, zonal_out.at[r], sem.at[r]))
        copies[-1].start()
    columns_s[...] = jnp.zeros_like(columns_s)
    columns_s[pl.ds(0, STEP), :] = edge_ref[...]
    across = columns_s[...].T[0:layers]
    at_edge = lax.broadcasted_iota(jnp.int32, across.shape, 1) == 127
    for r in range(rows):
        merid_s[r] = jnp.where(at_edge, pltpu.roll(across, 127 - r, 1), merid_ref[r])
    copies.append(pltpu.make_async_copy(merid_s, merid_out, sem.at[rows]))
    copies[-1].start()
    for copy in copies:
        copy.wait()


def correct_body(gathered_ref, tracer_ref, warmth_ref, tracers_out, warmth_out, new_s, heat_s, sem):
    tracers, rows = tracer_ref.shape[:2]
    totals = jnp.sum(gathered_ref[...], axis=0, keepdims=True)
    spread = [
        jnp.broadcast_to(totals[:, i : i + 1], (1, 128)) for i in range(tracers + 2)
    ]
    scale = 1.0 / spread[tracers + 1]
    copies = []
    for t in range(tracers):
        for r in range(rows):
            new_s[t, r] = tracer_ref[t, r] + spread[t] * scale
            copies.append(
                pltpu.make_async_copy(
                    new_s.at[t, r], tracers_out.at[t, r], sem.at[t * rows + r]
                )
            )
            copies[-1].start()
    heat_s[...] = warmth_ref[...] + spread[tracers] * (scale * (1.0 / HEAT))
    copies.append(pltpu.make_async_copy(heat_s, warmth_out, sem.at[tracers * rows]))
    copies[-1].start()
    for copy in copies:
        copy.wait()


def ring_shift(value, axis, steps):
    count = lax.axis_size(axis)
    return lax.ppermute(value, axis, [(i, (i + steps) % count) for i in range(count)])


def add_mirrored(value, axis):
    count = lax.axis_size(axis)
    return value + lax.ppermute(value, axis, [(i, count - 1 - i) for i in range(count)])


def sums_to_gather(sums):
    sums = add_mirrored(sums, "core")
    sums = add_mirrored(sums, ("z_hi", "z_lo"))
    count = lax.axis_size(CUBE)
    rows = jnp.broadcast_to(sums[None], (count, *sums.shape))
    return lax.all_to_all(rows, CUBE, 0, 0, tiled=True).reshape(count, 128)


def kernel(body, flops, moved, scratch, near, outs, operands):
    operands = [
        pltpu.with_memory_space_constraint(x, pltpu.VMEM if i in near else pltpu.HBM)
        for i, x in enumerate(operands)
    ]
    vmem = pl.BlockSpec(memory_space=pltpu.VMEM)
    hbm = pl.BlockSpec(memory_space=pl.ANY)
    return pl.pallas_call(
        body,
        out_shape=tuple(
            pltpu.VMEM(shape, jnp.float32)
            if place == "vmem"
            else jax.ShapeDtypeStruct(shape, jnp.float32)
            for shape, place in outs
        ),
        in_specs=[vmem] * len(operands),
        out_specs=tuple(hbm if place == "any" else vmem for _, place in outs),
        scratch_shapes=scratch,
        cost_estimate=pl.CostEstimate(flops=flops, bytes_accessed=moved, transcendentals=0),
        compiler_params=pltpu.CompilerParams(vmem_limit_bytes=24 * 2**20),
    )(*operands)


def local(species, zonal, merid, warmth, depth, level, start, end):
    tracers = species.shape[0]
    plane = rows, layers, columns = depth.shape
    tall = layers + 2 * PAD
    tile = (STEP, 128)
    real = functools.partial(pltpu.VMEM, dtype=jnp.float32)
    row_halo, column_halo = kernel(
        pack_body,
        100_000,
        600_000,
        [real((128, 128))],
        (),
        [((4, layers, columns), "vmem"), (tile, "vmem")],
        (depth, level, start, end),
    )
    column_halo = ring_shift(column_halo, GX, -1)
    row_halo = ring_shift(row_halo, GY, -1)
    tracer_new, warmth_new, zonal_part, merid_part, last, edge, parts = kernel(
        own_body,
        20_000_000,
        2_000_000,
        [
            real((rows, tall, columns)),
            real((rows, tall, columns)),
            real((rows, tall, columns)),
            real((rows, tall, columns)),
            real((tracers + 1, rows, tall, columns)),
            real(plane),
            real(plane),
            real((128, 128)),
        ],
        (),
        [
            ((tracers, *plane), "vmem"),
            (plane, "vmem"),
            (plane, "vmem"),
            (plane, "vmem"),
            ((3, layers, columns), "vmem"),
            (tile, "vmem"),
            ((2, *tile), "vmem"),
        ],
        (species, zonal, merid, warmth, depth, level, start, end),
    )
    merid_last, energy = kernel(
        functools.partial(east_first_body, layers),
        200_000,
        200_000,
        [],
        range(3),
        [(tile, "vmem"), (tile, "vmem")],
        (column_halo, edge, parts),
    )
    zonal_last, sums = kernel(
        functools.partial(north_last_body, tracers),
        2_000_000,
        500_000,
        [real((tall, columns)), real((tall, columns))],
        range(5),
        [((layers, columns), "vmem"), ((1, 128), "vmem")],
        (row_halo, zonal_part, last, parts, energy),
    )
    gathered = sums_to_gather(sums)
    zonal_new, merid_new = kernel(
        winds_body,
        200_000,
        700_000,
        [real(plane), real((128, 128)), pltpu.SemaphoreType.DMA((rows + 1,))],
        range(4),
        [(plane, "any"), (plane, "any")],
        (zonal_part, zonal_last, merid_part, merid_last),
    )
    tracers_out, warmth_out = kernel(
        correct_body,
        1_000_000,
        2_000_000,
        [real((tracers, *plane)), real(plane), pltpu.SemaphoreType.DMA((tracers * rows + 1,))],
        range(3),
        [((tracers, *plane), "any"), (plane, "any")],
        (gathered, tracer_new, warmth_new),
    )
    return tracers_out, zonal_new, merid_new, warmth_out


def solution(mesh):
    split = Mesh(mesh.devices.reshape(SPLIT), NAMES)
    plane = P(GY, None, GX)
    stack = P(None, GY, None, GX)
    return jax.shard_map(
        local,
        mesh=split,
        in_specs=(stack,) + (plane,) * 7,
        out_specs=(stack, plane, plane, plane),
        check_vma=False,
    )
```
